32 devices in a mesh: replica: 4 (over y, z), ep: 8 (over x, core).
Axes of the slice: x: 4, y: 2, z: 2, core: 2. Of those that a mesh axis runs over, the one named last changes fastest.
The devices are a block of a 4x4x8 slice.
Arguments:
- tok_in: bfloat16 [8192, 1024], P(('replica', 'ep')), parts along dimension 0
- routes: int32 [2, 8192, 8], P(None, ('replica', 'ep')), parts along dimension 1
- gate_vals: float32 [2, 8192, 8], P(None, ('replica', 'ep')), parts along dimension 1
- w_gate: bfloat16 [2, 64, 1024, 512], P(None, ('replica', 'ep')), parts along dimension 1
- w_up: bfloat16 [2, 64, 1024, 512], P(None, ('replica', 'ep')), parts along dimension 1
- w_down: bfloat16 [2, 64, 512, 1024], P(None, ('replica', 'ep')), parts along dimension 1
- sh_gate: bfloat16 [2, 1024, 512], replicated
- sh_up: bfloat16 [2, 1024, 512], replicated
- sh_down: bfloat16 [2, 512, 1024], replicated
- old_map: int32 [2, 64], P(None, 'replica'), parts along dimension 1
- move_slot: int32 [2, 8], P(None, 'replica'), parts along dimension 1
- move_expert: int32 [2, 8], P(None, 'replica'), parts along dimension 1
Outputs:
- output 1: bfloat16 [8192, 1024], P(('replica', 'ep')), parts along dimension 0
- output 2: bfloat16 [2, 64, 1024, 512], P(None, ('replica', 'ep')), parts along dimension 1
- output 3: bfloat16 [2, 64, 1024, 512], P(None, ('replica', 'ep')), parts along dimension 1
- output 4: bfloat16 [2, 64, 512, 1024], P(None, ('replica', 'ep')), parts along dimension 1
There are 4 independent parts. The reference program is written for one: setup_inputs(seed, part) draws one part's arguments, and reference() takes and returns one part's arrays. A program takes and returns all parts, laid end to end along the dimension named above; an argument that names none is the same for every part.
All inputs are finite; a program needn't handle non-finite values.
Results may differ from the reference program's by a relative error of at most 0.0115662.
Values are sent between devices in bfloat16 or wider.
A program may use at most 768 MiB of HBM per device.

```python
import jax
import jax.numpy as jnp
from jax import lax

HIDDEN = 1024
EXPERT_FF = 512
SHARED_FF = 512
TOP_K = 8
GROUP_DEVS = 8
SLOTS_DEV = 2
TOKENS_DEV = 256
MOVE_COUNT = 2
EXPERTS = 12

SLOT_COUNT = GROUP_DEVS * SLOTS_DEV
TOKEN_COUNT = GROUP_DEVS * TOKENS_DEV
SCORE_RANGE = 2 ** 10
HOT_BONUS = 2 ** 9
COVER_BONUS = 2 ** 12


def draw_layout(rng_key):
    perm_key, extra_key, place_key = jax.random.split(rng_key, 3)
    expert_perm = jax.random.permutation(perm_key, EXPERTS).astype(jnp.int32)
    extra_slot = jax.random.randint(extra_key, (SLOT_COUNT - EXPERTS,), 0, EXPERTS, dtype=jnp.int32)
    canon_old = jnp.concatenate([expert_perm, extra_slot])
    cycled = jnp.concatenate([expert_perm[1:MOVE_COUNT], expert_perm[:1]])
    slot_perm = jax.random.permutation(place_key, SLOT_COUNT).astype(jnp.int32)
    old_map = canon_old[slot_perm]
    slot_of_canon = jnp.argsort(slot_perm).astype(jnp.int32)
    return old_map, slot_of_canon[:MOVE_COUNT], cycled, expert_perm[:MOVE_COUNT]


def draw_routes(rng_key, hot_ids):
    score_key, offset_key = jax.random.split(rng_key)
    score_int = jax.random.randint(score_key, (TOKEN_COUNT, EXPERTS), 0, SCORE_RANGE, dtype=jnp.int32)
    expert_ids = jnp.arange(EXPERTS, dtype=jnp.int32)
    is_hot = jnp.any(expert_ids[:, None] == hot_ids[None, :], axis=1).astype(jnp.int32)
    offset = jax.random.randint(offset_key, (), 0, EXPERTS, dtype=jnp.int32)
    token_ids = jnp.arange(TOKEN_COUNT, dtype=jnp.int32)
    cover_mask = ((token_ids[:, None] + offset) % EXPERTS == expert_ids[None, :]).astype(jnp.int32)
    total_score = score_int + HOT_BONUS * is_hot[None, :] + COVER_BONUS * cover_mask
    picked = lax.top_k(total_score * EXPERTS + expert_ids[None, :], TOP_K)[1]
    return picked.astype(jnp.int32)


def place_slots(expert_w, slot_map):
    return jnp.take(expert_w, slot_map, axis=0)


def setup_inputs(seed: int = 0, part: int = 0) -> dict:
    base_key = jax.random.key(seed)
    part_key = jax.random.fold_in(base_key, part)
    draw_keys = jax.random.split(part_key, 7)
    shared_keys = jax.random.split(jax.random.key(seed + 1), 3)
    old_map, move_slot, move_expert, hot_ids = jax.vmap(draw_layout)(jax.random.split(draw_keys[0], 2))
    routes = jax.vmap(draw_routes)(jax.random.split(draw_keys[1], 2), hot_ids)
    gate_vals = (0.5 + jax.random.uniform(draw_keys[2], (2, TOKEN_COUNT, TOP_K))) / TOP_K ** 0.5
    tok_in = jax.random.normal(draw_keys[3], (TOKEN_COUNT, HIDDEN)).astype(jnp.bfloat16)
    gate_e = (jax.random.normal(draw_keys[4], (2, EXPERTS, HIDDEN, EXPERT_FF)) * HIDDEN ** -0.5).astype(jnp.bfloat16)
    up_e = (jax.random.normal(draw_keys[5], (2, EXPERTS, HIDDEN, EXPERT_FF)) * HIDDEN ** -0.5).astype(jnp.bfloat16)
    down_e = (jax.random.normal(draw_keys[6], (2, EXPERTS, EXPERT_FF, HIDDEN)) * EXPERT_FF ** -0.5).astype(jnp.bfloat16)
    sh_gate = (jax.random.normal(shared_keys[0], (2, HIDDEN, SHARED_FF)) * HIDDEN ** -0.5).astype(jnp.bfloat16)
    sh_up = (jax.random.normal(shared_keys[1], (2, HIDDEN, SHARED_FF)) * HIDDEN ** -0.5).astype(jnp.bfloat16)
    sh_down = (jax.random.normal(shared_keys[2], (2, SHARED_FF, HIDDEN)) * SHARED_FF ** -0.5).astype(jnp.bfloat16)
    return {
        'tok_in': tok_in,
        'routes': routes,
        'gate_vals': gate_vals,
        'w_gate': jax.vmap(place_slots)(gate_e, old_map),
        'w_up': jax.vmap(place_slots)(up_e, old_map),
        'w_down': jax.vmap(place_slots)(down_e, old_map),
        'sh_gate': sh_gate,
        'sh_up': sh_up,
        'sh_down': sh_down,
        'old_map': old_map,
        'move_slot': move_slot,
        'move_expert': move_expert,
    }


def first_holder(slot_map, wanted):
    slot_ids = jnp.arange(SLOT_COUNT, dtype=jnp.int32)
    hit_mask = slot_map[None, :] == wanted[:, None]
    return jnp.min(jnp.where(hit_mask, slot_ids[None, :], SLOT_COUNT), axis=1)


def swiglu(hidden, w_gate, w_up, w_down):
    gate_proj = jnp.dot(hidden, w_gate, preferred_element_type=jnp.float32)
    up_proj = jnp.dot(hidden, w_up, preferred_element_type=jnp.float32)
    inner_act = (jax.nn.silu(gate_proj) * up_proj).astype(jnp.bfloat16)
    return jnp.dot(inner_act, w_down, preferred_element_type=jnp.float32)


def moe_layer(hidden, route_ids, gate_w, w_gate, w_up, w_down, sh_gate, sh_up, sh_down, slot_map):
    expert_ids = jnp.arange(EXPERTS, dtype=jnp.int32)
    holders = first_holder(slot_map, expert_ids)

    def add_expert(running, expert_idx):
        holder_slot = holders[expert_idx]
        expert_out = swiglu(hidden, w_gate[holder_slot], w_up[holder_slot], w_down[holder_slot])
        gate_col = jnp.sum(jnp.where(route_ids == expert_idx, gate_w, 0.0), axis=1)
        return running + gate_col[:, None] * expert_out, None

    start_acc = hidden.astype(jnp.float32) + swiglu(hidden, sh_gate, sh_up, sh_down)
    total_out = lax.scan(add_expert, start_acc, expert_ids)[0]
    return total_out.astype(jnp.bfloat16)


def reference(tok_in, routes, gate_vals, w_gate, w_up, w_down, sh_gate, sh_up, sh_down, old_map, move_slot, move_expert):
    hidden = tok_in
    new_sets = []
    for layer_idx in range(2):
        hidden = moe_layer(hidden, routes[layer_idx], gate_vals[layer_idx], w_gate[layer_idx], w_up[layer_idx], w_down[layer_idx], sh_gate[layer_idx], sh_up[layer_idx], sh_down[layer_idx], old_map[layer_idx])
        new_map = old_map[layer_idx].at[move_slot[layer_idx]].set(move_expert[layer_idx])
        source = first_holder(old_map[layer_idx], new_map)
        new_sets.append((jnp.take(w_gate[layer_idx], source, axis=0), jnp.take(w_up[layer_idx], source, axis=0), jnp.take(w_down[layer_idx], source, axis=0)))
    new_gate = jnp.stack([new_sets[0][0], new_sets[1][0]])
    new_up = jnp.stack([new_sets[0][1], new_sets[1][1]])
    new_down = jnp.stack([new_sets[0][2], new_sets[1][2]])
    return (hidden, new_gate, new_up, new_down)
```

```python
import functools

import jax
import jax.numpy as jnp
from jax import lax
from jax.experimental import pallas as pl
from jax.experimental.pallas import tpu as pltpu
from jax.sharding import PartitionSpec as P

TOKEN_AXES = ('replica', 'ep')
MESH = pl.DeviceIdType.MESH
CHUNKS = 4
PIECE = 16
LAG = 2
SEND_SLOTS = 4
OUT_SLOTS = 4
RECV_SEMS = 8
RECV_SLOTS = 16
LAYERS = 2
PLACE = {'u1': (2, 2), 'u2': (2, 2), 'u3': (2, 2), 'own': (2, 2), 'sum': (1, 1), 'fin': (1, 1)}


def kernel(n_chip, dims, tab, coef, tok, wg, wu, wd, sg, su, sd,
           tok_out, w_out,
           wall, shw, tbuf, pbuf, rpure, ropp, rsum, crecv, mrecv, msend, mout,
           own_sem, w_send, w_recv, sh_sem, tok_sem, c_send, c_recv,
           ag_send, ag_recv, rl_send, rl_recv, pu_send, pu_recv,
           op_send, op_recv, sm_send, sm_recv,
           mv_send, mv_recv, mo_local, mo_send, mo_recv):
    toks, d_model, d_ff = dims
    half = toks // 2
    ch = half // CHUNKS
    quarter = d_model // 4
    per_phase = quarter // PIECE
    n_piece = 3 * per_phase
    n_step = n_piece + 2 * LAG
    f32, bf16 = jnp.float32, jnp.bfloat16

    me = lax.axis_index('ep')
    chip = me // 2
    core = lax.rem(me, 2)
    dev_r = lax.rem(chip + 1, n_chip) * 2 + core
    dev_l = lax.rem(chip + n_chip - 1, n_chip) * 2 + core
    dev_o = lax.rem(chip + 2, n_chip) * 2 + core
    dev_p = chip * 2 + 1 - core

    def rdma(src, dst, ss, rs, dev):
        return pltpu.make_async_remote_copy(src_ref=src, dst_ref=dst, send_sem=ss, recv_sem=rs,
                                            device_id={'ep': dev}, device_id_type=MESH)

    base = core * 2
    mine = pl.ds(base, 2)
    loads = []

    def weight_parts(l, g, u, d):
        return [(g, pl.ds(0, d_model), None), (u, pl.ds(d_model, d_model), None),
                (d, pl.ds(2 * d_model, d_ff), 0), (d, pl.ds(2 * d_model + d_ff, d_ff), 1)]

    def src_of(ref, col, l):
        if col is None:
            return ref.at[l]
        cols = pl.ds(col * d_ff, d_ff)
        return ref.at[l, :, :, cols] if len(ref.shape) == 4 else ref.at[l, :, cols]

    def own_load(l):
        return [pltpu.make_async_copy(src_of(r, c, l), wall.at[l, mine, rows, :], own_sem.at[l, i])
                for i, (r, rows, c) in enumerate(weight_parts(l, wg, wu, wd))]

    def shared_load(l):
        return [pltpu.make_async_copy(src_of(r, c, l), shw.at[l, rows, :], sh_sem.at[l, i])
                for i, (r, rows, c) in enumerate(weight_parts(l, sg, su, sd))]

    def partner_load(l):
        return [rdma(src_of(r, c, l), wall.at[l, mine, rows, :], w_send.at[l, i], w_recv.at[l, i], dev_p)
                for i, (r, rows, c) in enumerate(weight_parts(l, wg, wu, wd))]

    tok_load = pltpu.make_async_copy(tok, tbuf.at[0, 0], tok_sem)
    tok_load.start()
    for c in own_load(0):
        c.start()

    barrier = pltpu.get_barrier_semaphore()
    for dev in (dev_l, dev_r, dev_o, dev_p):
        pl.semaphore_signal(barrier, inc=1, device_id={'ep': dev}, device_id_type=MESH)
    pl.semaphore_wait(barrier, 4)

    def ag_copies(l, c, src, kinds):
        lo, hi = pl.ds(c * ch, ch), pl.ds(half + c * ch, ch)
        form = [(lo, 1, lo, dev_r), (hi, 2, lo, dev_r), (hi, 1, hi, dev_l), (lo, 2, hi, dev_l)]
        return [rdma(src.at[form[k][0], :], tbuf.at[l, form[k][1], form[k][2], :],
                     ag_send.at[l, k, c], ag_recv.at[l, k, c], form[k][3]) for k in kinds]

    def ag_start(l, src, c_list, kinds):
        for c in c_list:
            for cp in ag_copies(l, c, src, kinds):
                cp.start()

    def relay(l, c, side):
        rows = pl.ds(c * ch, ch) if side == 0 else pl.ds(half + c * ch, ch)
        dev = dev_r if side == 0 else dev_l
        return rdma(tbuf.at[l, 1, rows, :], tbuf.at[l, 3, rows, :], rl_send.at[l, side, c], rl_recv.at[l, side, c], dev)

    ag_start(0, tok, range(CHUNKS), (0, 2))
    cl = lax.rem(chip + n_chip - 1, n_chip)
    cr = lax.rem(chip + 1, n_chip)
    co = lax.rem(chip + 2, n_chip)
    coefs = [rdma(coef.at[cr], crecv.at[0], c_send.at[0], c_recv.at[0], dev_r),
             rdma(coef.at[cl], crecv.at[1], c_send.at[1], c_recv.at[1], dev_l),
             rdma(coef.at[co], crecv.at[2], c_send.at[2], c_recv.at[2], dev_o)]
    for c in coefs:
        c.start()
    for c in partner_load(0):
        c.start()
    ag_start(0, tok, range(CHUNKS), (1, 3))
    for c in shared_load(0) + own_load(1):
        c.start()
    for c in partner_load(1):
        c.start()
    for c in shared_load(1):
        c.start()

    eye = lax.broadcasted_iota(jnp.int32, (half, half), 0) == lax.broadcasted_iota(jnp.int32, (half, half), 1)

    def column(row):
        return jnp.sum(jnp.where(eye, jnp.broadcast_to(row, (half, half)), 0.0), axis=1, keepdims=True)

    def gates(l, u, q):
        s = l * 4 + q
        lo, hi = pl.ds(0, half), pl.ds(half, half)
        if u == 0:
            a, b = coef[chip, s, :, lo], coef[chip, s, :, hi]
        elif u == 1:
            a, b = crecv[0, s, :, lo], crecv[1, s, :, hi]
        elif u == 2:
            a, b = crecv[0, s, :, hi], crecv[1, s, :, lo]
        else:
            a, b = crecv[2, s, :, lo], crecv[2, s, :, hi]
        return jnp.concatenate([column(a), column(b)], axis=0)

    def swiglu(x, w):
        g = jnp.dot(x, w[pl.ds(0, d_model), :], preferred_element_type=f32)
        u = jnp.dot(x, w[pl.ds(d_model, d_model), :], preferred_element_type=f32)
        inner = (jax.nn.silu(g) * u).astype(bf16)
        return [jnp.dot(inner, w[pl.ds(2 * d_model + j * d_ff, d_ff), :], preferred_element_type=f32) for j in range(2)]

    def unit(l, u):
        def one(q, carry):
            outs = swiglu(tbuf[l, u], wall.at[l, q])
            col = gates(l, u, q)
            for j in range(2):
                cols = pl.ds(j * d_ff, d_ff)
                pbuf[u, :, cols] = pbuf[u, :, cols] + col * outs[j]
            return carry

        if u == 0:
            x = tbuf[l, 0]
            outs = swiglu(x, shw.at[l])
            for j in range(2):
                pbuf[0, :, j * d_ff:(j + 1) * d_ff] = x[:, j * d_ff:(j + 1) * d_ff].astype(f32) + outs[j]
        else:
            pbuf[u] = jnp.zeros(pbuf.shape[1:], f32)
        lax.fori_loop(0, 4, one, 0)

    info = []
    for m in range(2 * LAYERS):
        s, t = tab[m], tab[4 + m]
        s_chip, s_loc = s >> 2, s & 3
        t_chip, t_loc = t >> 2, t & 3
        dist = [(t_chip - s_chip) & (n_chip - 1), (s_chip - t_chip) & (n_chip - 1)]
        info.append((m // 2, s_loc, s_chip == chip, dist, t_chip == chip, t_loc))

    def piece_row(i, d):
        if isinstance(i, int):
            ph, rest = i // per_phase, i % per_phase
        else:
            ph, rest = lax.div(i, per_phase), lax.rem(i, per_phase)
        return pl.multiple_of(ph * d_model + core * 2 * quarter + d * quarter + rest * PIECE, PIECE)

    def mod(k, n):
        return k % n if isinstance(k, int) else lax.rem(k, n)

    def move_copy(k, d):
        slot = mod(k, SEND_SLOTS)
        return rdma(msend.at[d, slot], mrecv.at[d, mod(k, RECV_SLOTS)], mv_send.at[d, slot], mv_recv.at[d, mod(k, RECV_SEMS)],
                    dev_r if d == 0 else dev_l)

    def out_copies(i, d):
        slot = mod(i, OUT_SLOTS)
        rows = pl.ds(piece_row(i, d), PIECE)
        own = pltpu.make_async_copy(mout.at[slot, d, 0], w_out.at[:, :, rows, :], mo_local.at[slot, d])
        far = rdma(mout.at[slot, d, 1], w_out.at[:, :, rows, :], mo_send.at[slot, d], mo_recv, dev_p)
        return own, far

    def pick(options, which):
        v = options[0]
        for q in range(1, 4):
            v = jnp.where(which == q, options[q], v)
        return v

    def emit(i, reuse):
        slot = mod(i, OUT_SLOTS)
        for d in range(2):
            if reuse:
                own, far = out_copies(i - OUT_SLOTS, d)
                own.wait()
                far.wait_send()
            rows = pl.ds(piece_row(i, d), PIECE)
            held = [[wall[l, q, rows, :] for q in range(4)] for l in range(LAYERS)]
            near = [[wall[l, base + j, rows, :] for j in range(2)] for l in range(LAYERS)]
            away = [[wall[l, 2 - base + j, rows, :] for j in range(2)] for l in range(LAYERS)]
            vals = []
            for m, (l, s_loc, _, dist, _, _) in enumerate(info):
                h = dist[d]
                v = pick(held[l], s_loc)
                for j in range(3):
                    v = jnp.where(h == j + 1, mrecv[d, mod(i + j * LAG, RECV_SLOTS), m], v)
                vals.append(v)
            for which in range(2):
                for j in range(2):
                    q = base + j if which == 0 else 2 - base + j
                    for l in range(LAYERS):
                        v = (away if which else near)[l][j]
                        for m in (2 * l, 2 * l + 1):
                            hit = jnp.logical_and(info[m][4], info[m][5] == q)
                            v = jnp.where(hit, vals[m], v)
                        mout[slot, d, which, l, j] = v
            own, far = out_copies(i, d)
            own.start()
            far.start()

    def step(k, has_own, has_in, reuse_send, emits, reuse_out):
        if has_in:
            for d in range(2):
                move_copy(k - LAG, d).wait_recv()
        if has_own or has_in == 1:
            slot = mod(k, SEND_SLOTS)
            for d in range(2):
                if reuse_send:
                    move_copy(k - SEND_SLOTS, d).wait_send()
                if has_own:
                    rows = pl.ds(piece_row(k, d), PIECE)
                    held = [[wall[l, q, rows, :] for q in range(4)] for l in range(LAYERS)]
                for m, (l, s_loc, is_src, _, _, _) in enumerate(info):
                    if has_own:
                        v = pick(held[l], s_loc)
                        if has_in:
                            v = jnp.where(is_src, v, mrecv[d, mod(k - LAG, RECV_SLOTS), m])
                    else:
                        v = mrecv[d, mod(k - LAG, RECV_SLOTS), m]
                    msend[d, slot, m] = v
                move_copy(k, d).start()
        if emits:
            emit(k - 3 * LAG, reuse_out)

    first_full = 3 * LAG + OUT_SLOTS

    def one_step(k):
        if k < n_step:
            step(k, k < n_piece, 1 if k >= LAG else 0, k >= SEND_SLOTS, k >= 3 * LAG, k >= first_full)
        else:
            step(k, False, 2, False, k >= 3 * LAG, k >= first_full)

    cursor = [0]

    def moves(count):
        a = cursor[0]
        b = min(a + count, n_step + LAG)
        cursor[0] = b
        k = a
        while k < b and k < first_full:
            one_step(k)
            k += 1
        mid = min(b, n_piece)
        if k < mid:
            def loop_body(kk, carry):
                step(kk, True, 1, True, True, True)
                return carry
            lax.fori_loop(k, mid, loop_body, 0)
            k = mid
        while k < b:
            one_step(k)
            k += 1

    for l in range(LAYERS):
        for c in range(CHUNKS):
            for cp in ag_copies(l, c, tbuf.at[l, 0], (0, 2)):
                cp.wait_recv()
            relay(l, c, 0).start()
            relay(l, c, 1).start()
        if l == 0:
            for c in own_load(0):
                c.wait()
            for c in partner_load(0):
                c.wait_recv()
            for c in coefs:
                c.wait_recv()
        lo, hi = pl.ds(0, half), pl.ds(half, half)

        def pure(ll):
            return [rdma(pbuf.at[1, lo, :], rpure.at[ll, lo, :], pu_send.at[ll, 0], pu_recv.at[ll, 0], dev_l),
                    rdma(pbuf.at[1, hi, :], rpure.at[ll, hi, :], pu_send.at[ll, 1], pu_recv.at[ll, 1], dev_r)]

        def opp(ll, c):
            a, b = pl.ds(c * ch, ch), pl.ds(half + c * ch, ch)
            return [rdma(pbuf.at[3, a, :], ropp.at[ll, b, :], op_send.at[ll, 0, c], op_recv.at[ll, 0, c], dev_r),
                    rdma(pbuf.at[3, b, :], ropp.at[ll, a, :], op_send.at[ll, 1, c], op_recv.at[ll, 1, c], dev_l)]

        def summed(ll, c):
            a, b = pl.ds(c * ch, ch), pl.ds(half + c * ch, ch)
            return [rdma(pbuf.at[2, a, :], rsum.at[ll, b, :], sm_send.at[ll, 0, c], sm_recv.at[ll, 0, c], dev_l),
                    rdma(pbuf.at[2, b, :], rsum.at[ll, a, :], sm_send.at[ll, 1, c], sm_recv.at[ll, 1, c], dev_r)]

        if l > 0:
            for cp in pure(l - 1):
                cp.wait_send()
        unit(l, 1)
        for cp in pure(l):
            cp.start()
        if l == 0:
            for c in own_load(1):
                c.wait()
            for c in partner_load(1):
                c.wait_recv()
        moves(PLACE['u1'][l])
        for c in range(CHUNKS):
            for cp in ag_copies(l, c, tbuf.at[l, 0], (1, 3)):
                cp.wait_recv()
            if l > 0:
                for cp in summed(l - 1, c):
                    cp.wait_send()
        unit(l, 2)
        moves(PLACE['u2'][l])
        for c in range(CHUNKS):
            relay(l, c, 0).wait_recv()
            relay(l, c, 1).wait_recv()
            if l > 0:
                for cp in opp(l - 1, c):
                    cp.wait_send()
        unit(l, 3)
        for c in range(CHUNKS):
            for cp in opp(l, c):
                cp.start()
        moves(PLACE['u3'][l])
        if l == 0:
            tok_load.wait()
        for c in shared_load(l):
            c.wait()
        unit(l, 0)
        moves(PLACE['own'][l])
        for c in range(CHUNKS):
            a, b = pl.ds(c * ch, ch), pl.ds(half + c * ch, ch)
            for cp in opp(l, c):
                cp.wait_recv()
            for rows in (a, b):
                pbuf[2, rows, :] = pbuf[2, rows, :] + ropp[l, rows, :]
            for cp in summed(l, c):
                cp.start()
            moves(PLACE['sum'][l])
        for cp in pure(l):
            cp.wait_recv()
        for c in range(CHUNKS):
            a, b = pl.ds(c * ch, ch), pl.ds(half + c * ch, ch)
            for cp in summed(l, c):
                cp.wait_recv()
            for rows in (a, b):
                new = (pbuf[0, rows, :] + rpure[l, rows, :] + rsum[l, rows, :]).astype(bf16)
                if l + 1 < LAYERS:
                    tbuf[l + 1, 0, rows, :] = new
                else:
                    tok_out[rows, :] = new
            if l + 1 < LAYERS:
                ag_start(l + 1, tbuf.at[l + 1, 0], [c], (0, 1, 2, 3))
            moves(PLACE['fin'][l])

    moves(n_step + LAG)

    for k in range(n_step - SEND_SLOTS, n_step):
        for d in range(2):
            move_copy(k, d).wait_send()
    for i in range(n_piece - OUT_SLOTS, n_piece):
        for d in range(2):
            own, far = out_copies(i, d)
            own.wait()
            far.wait_send()
    arrived = w_out.at[:, :, pl.ds(0, 6 * quarter), :]
    pltpu.make_async_copy(arrived, arrived, mo_recv).wait()
    last = LAYERS - 1
    for cp in pure(last):
        cp.wait_send()
    for c in range(CHUNKS):
        for cp in opp(last, c) + summed(last, c):
            cp.wait_send()
    for l in range(LAYERS):
        for c in range(CHUNKS):
            for cp in ag_copies(l, c, tok if l == 0 else tbuf.at[l, 0], (0, 1, 2, 3)):
                cp.wait_send()
            relay(l, c, 0).wait_send()
            relay(l, c, 1).wait_send()
        for cp in partner_load(l):
            cp.wait_send()
    for cp in coefs:
        cp.wait_send()


def fused(n_ep, tab, coef, tok, wg, wu, wd, sg, su, sd):
    toks, d_model = tok.shape
    d_ff = sg.shape[-1]
    n_chip = n_ep // 2
    rows = 3 * d_model
    f32, bf16 = jnp.float32, jnp.bfloat16
    any_spec = pl.BlockSpec(memory_space=pl.ANY)
    vmem = pl.BlockSpec(memory_space=pltpu.VMEM)
    dma = pltpu.SemaphoreType.DMA
    return pl.pallas_call(
        functools.partial(kernel, n_chip, (toks, d_model, d_ff)),
        out_shape=(jax.ShapeDtypeStruct((toks, d_model), bf16),
                   jax.ShapeDtypeStruct((LAYERS, 2, rows, d_ff), bf16)),
        in_specs=[pl.BlockSpec(memory_space=pltpu.SMEM), vmem] + [any_spec] * 7,
        out_specs=(vmem, any_spec),
        scratch_shapes=[
            pltpu.VMEM((LAYERS, 4, rows, d_ff), bf16),
            pltpu.VMEM((LAYERS, rows, d_ff), bf16),
            pltpu.VMEM((LAYERS, 4, toks, d_model), bf16),
            pltpu.VMEM((4, toks, d_model), f32),
            pltpu.VMEM((LAYERS, toks, d_model), f32),
            pltpu.VMEM((LAYERS, toks, d_model), f32),
            pltpu.VMEM((LAYERS, toks, d_model), f32),
            pltpu.VMEM((3,) + coef.shape[1:], f32),
            pltpu.VMEM((2, RECV_SLOTS, 4, PIECE, d_ff), bf16),
            pltpu.VMEM((2, SEND_SLOTS, 4, PIECE, d_ff), bf16),
            pltpu.VMEM((OUT_SLOTS, 2, 2, LAYERS, 2, PIECE, d_ff), bf16),
            dma((LAYERS, 4)), dma((LAYERS, 4)), dma((LAYERS, 4)), dma((LAYERS, 4)), dma(()), dma((3,)), dma((3,)),
            dma((LAYERS, 4, CHUNKS)), dma((LAYERS, 4, CHUNKS)), dma((LAYERS, 2, CHUNKS)), dma((LAYERS, 2, CHUNKS)),
            dma((LAYERS, 2)), dma((LAYERS, 2)),
            dma((LAYERS, 2, CHUNKS)), dma((LAYERS, 2, CHUNKS)), dma((LAYERS, 2, CHUNKS)), dma((LAYERS, 2, CHUNKS)),
            dma((2, SEND_SLOTS)), dma((2, RECV_SEMS)), dma((OUT_SLOTS, 2)), dma((OUT_SLOTS, 2)), dma(()),
        ],
        compiler_params=pltpu.CompilerParams(collective_id=0, has_side_effects=True, vmem_limit_bytes=67043328),
    )(tab, coef, tok, wg, wu, wd, sg, su, sd)


def solution(mesh):
    n_ep = mesh.shape['ep']

    def body(tok_in, routes, gate_vals, w_gate, w_up, w_down, sh_gate, sh_up, sh_down, old_map, move_slot, move_expert):
        n_slot = old_map.shape[1]
        slot_ids = jnp.arange(n_slot, dtype=jnp.int32)
        same = old_map[:, :, None] == old_map[:, None, :]
        serve = jnp.min(jnp.where(same, slot_ids[None, None, :], n_slot), axis=2) == slot_ids[None, :]
        served = jnp.where(serve, old_map, -1)
        hit = routes.transpose(0, 2, 1)[:, None] == served[:, :, None, None]
        coef = jnp.sum(jnp.where(hit, gate_vals.transpose(0, 2, 1)[:, None], 0.0), axis=2)
        coef = coef.reshape(LAYERS, n_slot // 4, 4, 1, -1).transpose(1, 0, 2, 3, 4)
        coef = coef.reshape(n_slot // 4, LAYERS * 4, 1, -1)
        holds = old_map[:, None, :] == move_expert[:, :, None]
        source = jnp.min(jnp.where(holds, slot_ids[None, None, :], n_slot), axis=2)
        tab = jnp.concatenate([source.reshape(-1), move_slot.reshape(-1)]).astype(jnp.int32)
        tok, packed = fused(n_ep, tab, coef, tok_in, w_gate, w_up, w_down, sh_gate, sh_up, sh_down)
        d_model, d_ff = w_gate.shape[2:]
        new_gate = packed[:, :, :d_model]
        new_up = packed[:, :, d_model:2 * d_model]
        new_down = jnp.concatenate([packed[:, :, 2 * d_model:2 * d_model + d_ff], packed[:, :, 2 * d_model + d_ff:]], axis=3)
        return (tok, new_gate, new_up, new_down)

    weight_spec = P(None, TOKEN_AXES, None, None)
    route_spec = P(None, TOKEN_AXES, None)
    map_spec = P(None, 'replica')
    shared_spec = P(None, None, None)
    tok_spec = P(TOKEN_AXES, None)
    return jax.shard_map(body, mesh=mesh, in_specs=(tok_spec, route_spec, route_spec, weight_spec, weight_spec, weight_spec, shared_spec, shared_spec, shared_spec, map_spec, map_spec, map_spec), out_specs=(tok_spec, weight_spec, weight_spec, weight_spec), check_vma=False)
```

```python
import functools

import jax
import jax.numpy as jnp
from jax import lax
from jax.experimental import pallas as pl
from jax.experimental.pallas import tpu as pltpu
from jax.sharding import PartitionSpec as P

TOKEN_AXES = ('replica', 'ep')
MESH = pl.DeviceIdType.MESH
CHUNKS = 4
PIECE = 16
LAG = 4
SEND_SLOTS = LAG + 2
OUT_SLOTS = 4
RECV_SEMS = 4 * LAG
RECV_SLOTS = 6 * LAG + 2
LAYERS = 2
PLACE = {'relay': (0, 0), 'u1': (0, 4), 'u2': (0, 4), 'u3': (2, 4), 'own': (4, 4), 'sum': (2, 2), 'fin': (2, 1)}


def kernel(n_chip, dims, old_map, move_slot, move_expert, routes, gate_vals, tok, wg, wu, wd, sg, su, sd,
           tok_out, og, ou, od,
           wall, shw, tbuf, pbuf, rpure, ropp, rsum, coef, crecv, mrecv, msend, mout,
           own_sem, w_send, w_recv, sh_sem, tok_sem, c_send, c_recv,
           ag_send, ag_recv, rl_send, rl_recv, pu_send, pu_recv,
           op_send, op_recv, sm_send, sm_recv,
           mv_send, mv_recv, mo_local, mo_send, mo_recv):
    toks, d_model, d_ff = dims
    half = toks // 2
    ch = half // CHUNKS
    quarter = d_model // 4
    per_phase = quarter // PIECE
    n_piece = 3 * per_phase
    n_step = n_piece + 2 * LAG
    f32, bf16 = jnp.float32, jnp.bfloat16

    me = lax.axis_index('ep')
    chip = me // 2
    core = lax.rem(me, 2)
    dev_r = lax.rem(chip + 1, n_chip) * 2 + core
    dev_l = lax.rem(chip + n_chip - 1, n_chip) * 2 + core
    dev_o = lax.rem(chip + 2, n_chip) * 2 + core
    dev_p = chip * 2 + 1 - core

    def rdma(src, dst, ss, rs, dev):
        return pltpu.make_async_remote_copy(src_ref=src, dst_ref=dst, send_sem=ss, recv_sem=rs,
                                            device_id={'ep': dev}, device_id_type=MESH)

    base = core * 2
    mine = pl.ds(base, 2)
    loads = []

    def weight_parts(l, g, u, d):
        return [(g, pl.ds(0, d_model), None), (u, pl.ds(d_model, d_model), None),
                (d, pl.ds(2 * d_model, d_ff), 0), (d, pl.ds(2 * d_model + d_ff, d_ff), 1)]

    def src_of(ref, col, l):
        if col is None:
            return ref.at[l]
        cols = pl.ds(col * d_ff, d_ff)
        return ref.at[l, :, :, cols] if len(ref.shape) == 4 else ref.at[l, :, cols]

    def own_load(l):
        return [pltpu.make_async_copy(src_of(r, c, l), wall.at[l, mine, rows, :], own_sem.at[l, i])
                for i, (r, rows, c) in enumerate(weight_parts(l, wg, wu, wd))]

    def shared_load(l):
        return [pltpu.make_async_copy(src_of(r, c, l), shw.at[l, rows, :], sh_sem.at[l, i])
                for i, (r, rows, c) in enumerate(weight_parts(l, sg, su, sd))]

    def partner_load(l):
        return [rdma(src_of(r, c, l), wall.at[l, mine, rows, :], w_send.at[l, i], w_recv.at[l, i], dev_p)
                for i, (r, rows, c) in enumerate(weight_parts(l, wg, wu, wd))]

    tok_load = pltpu.make_async_copy(tok, tbuf.at[0, 0], tok_sem)
    tok_load.start()
    for c in own_load(0):
        c.start()

    n_slot = n_chip * 4
    for l in range(LAYERS):
        ids = [old_map[l, q] for q in range(n_slot)]
        for q in range(n_slot):
            want = ids[q]
            for p in range(q):
                want = jnp.where(ids[p] == ids[q], -1, want)
            row = jnp.sum(jnp.where(routes[l] == want, gate_vals[l], 0.0), axis=0, keepdims=True)
            coef[q // 4, l * 4 + q % 4] = row

    barrier = pltpu.get_barrier_semaphore()
    for dev in (dev_l, dev_r, dev_o, dev_p):
        pl.semaphore_signal(barrier, inc=1, device_id={'ep': dev}, device_id_type=MESH)
    pl.semaphore_wait(barrier, 4)

    def ag_copies(l, c, src, kinds):
        lo, hi = pl.ds(c * ch, ch), pl.ds(half + c * ch, ch)
        form = [(lo, 1, lo, dev_r), (hi, 2, lo, dev_r), (hi, 1, hi, dev_l), (lo, 2, hi, dev_l)]
        return [rdma(src.at[form[k][0], :], tbuf.at[l, form[k][1], form[k][2], :],
                     ag_send.at[l, k, c], ag_recv.at[l, k, c], form[k][3]) for k in kinds]

    def ag_start(l, src, c_list, kinds):
        for c in c_list:
            for cp in ag_copies(l, c, src, kinds):
                cp.start()

    def relay(l, c, side):
        rows = pl.ds(c * ch, ch) if side == 0 else pl.ds(half + c * ch, ch)
        dev = dev_r if side == 0 else dev_l
        return rdma(tbuf.at[l, 1, rows, :], tbuf.at[l, 3, rows, :], rl_send.at[l, side, c], rl_recv.at[l, side, c], dev)

    ag_start(0, tok, range(CHUNKS), (0, 2))
    cl = lax.rem(chip + n_chip - 1, n_chip)
    cr = lax.rem(chip + 1, n_chip)
    co = lax.rem(chip + 2, n_chip)
    coefs = [rdma(coef.at[cr], crecv.at[0], c_send.at[0], c_recv.at[0], dev_r),
             rdma(coef.at[cl], crecv.at[1], c_send.at[1], c_recv.at[1], dev_l),
             rdma(coef.at[co], crecv.at[2], c_send.at[2], c_recv.at[2], dev_o)]
    for c in coefs:
        c.start()
    for c in partner_load(0):
        c.start()
    ag_start(0, tok, range(CHUNKS), (1, 3))
    for c in shared_load(0) + own_load(1):
        c.start()
    for c in partner_load(1):
        c.start()
    for c in shared_load(1):
        c.start()

    eye = lax.broadcasted_iota(jnp.int32, (half, half), 0) == lax.broadcasted_iota(jnp.int32, (half, half), 1)

    def column(row):
        return jnp.sum(jnp.where(eye, jnp.broadcast_to(row, (half, half)), 0.0), axis=1, keepdims=True)

    def gates(l, u, q):
        s = l * 4 + q
        lo, hi = pl.ds(0, half), pl.ds(half, half)
        if u == 0:
            a, b = coef[chip, s, :, lo], coef[chip, s, :, hi]
        elif u == 1:
            a, b = crecv[0, s, :, lo], crecv[1, s, :, hi]
        elif u == 2:
            a, b = crecv[0, s, :, hi], crecv[1, s, :, lo]
        else:
            a, b = crecv[2, s, :, lo], crecv[2, s, :, hi]
        return jnp.concatenate([column(a), column(b)], axis=0)

    def swiglu(x, w):
        g = jnp.dot(x, w[pl.ds(0, d_model), :], preferred_element_type=f32)
        u = jnp.dot(x, w[pl.ds(d_model, d_model), :], preferred_element_type=f32)
        inner = (jax.nn.silu(g) * u).astype(bf16)
        return [jnp.dot(inner, w[pl.ds(2 * d_model + j * d_ff, d_ff), :], preferred_element_type=f32) for j in range(2)]

    info = []
    for m in range(2 * LAYERS):
        t, want = move_slot[m // 2, m % 2], move_expert[m // 2, m % 2]
        s = jnp.int32(0)
        for q in range(n_slot - 1, 0, -1):
            s = jnp.where(old_map[m // 2, q] == want, q, s)
        s_chip, s_loc = s >> 2, s & 3
        t_chip, t_loc = t >> 2, t & 3
        dist = [(t_chip - s_chip) & (n_chip - 1), (s_chip - t_chip) & (n_chip - 1)]
        info.append((m // 2, s_loc, s_chip == chip, dist, t_chip == chip, t_loc))

    def piece_row(i, d):
        if isinstance(i, int):
            ph, rest = i // per_phase, i % per_phase
        else:
            ph, rest = lax.div(i, per_phase), lax.rem(i, per_phase)
        return pl.multiple_of(ph * d_model + core * 2 * quarter + d * quarter + rest * PIECE, PIECE)

    def mod(k, n):
        return k % n if isinstance(k, int) else lax.rem(k, n)

    def move_copy(k, d):
        slot = mod(k, SEND_SLOTS)
        return rdma(msend.at[d, slot], mrecv.at[d, mod(k, RECV_SLOTS)], mv_send.at[d, slot], mv_recv.at[d, mod(k, RECV_SEMS)],
                    dev_r if d == 0 else dev_l)

    def out_copies(i, d, ph=0):
        slot = mod(i, OUT_SLOTS)
        row = d * quarter + mod(i, per_phase) * PIECE
        if ph < 2:
            dst = (og, ou)[ph].at[:, :, pl.ds(pl.multiple_of(row + core * 2 * quarter, PIECE), PIECE), :]
        else:
            dst = od.at[:, :, pl.ds(pl.multiple_of(row, PIECE), PIECE), pl.ds(pl.multiple_of(core * d_ff, d_ff), d_ff)]
        own = pltpu.make_async_copy(mout.at[slot, d, 0], dst, mo_local.at[slot, d])
        far = rdma(mout.at[slot, d, 1], dst, mo_send.at[slot, d], mo_recv.at[ph], dev_p)
        return own, far

    def pick(options, which):
        v = options[0]
        for q in range(1, 4):
            v = jnp.where(which == q, options[q], v)
        return v

    def emit(i, reuse, ph):
        slot = mod(i, OUT_SLOTS)
        for d in range(2):
            if reuse:
                own, far = out_copies(i - OUT_SLOTS, d)
                own.wait()
                far.wait_send()
            rows = pl.ds(piece_row(i, d), PIECE)
            held = [[wall[l, q, rows, :] for q in range(4)] for l in range(LAYERS)]
            near = [[wall[l, base + j, rows, :] for j in range(2)] for l in range(LAYERS)]
            away = [[wall[l, 2 - base + j, rows, :] for j in range(2)] for l in range(LAYERS)]
            vals = []
            for m, (l, s_loc, _, dist, _, _) in enumerate(info):
                h = dist[d]
                v = pick(held[l], s_loc)
                for j in range(3):
                    v = jnp.where(h == j + 1, mrecv[d, mod(i + j * LAG, RECV_SLOTS), m], v)
                vals.append(v)
            for which in range(2):
                for j in range(2):
                    q = base + j if which == 0 else 2 - base + j
                    for l in range(LAYERS):
                        v = (away if which else near)[l][j]
                        for m in (2 * l, 2 * l + 1):
                            hit = jnp.logical_and(info[m][4], info[m][5] == q)
                            v = jnp.where(hit, vals[m], v)
                        mout[slot, d, which, l, j] = v
            own, far = out_copies(i, d, ph)
            own.start()
            far.start()

    def step(k, has_own, has_in, reuse_send, emits, reuse_out, ph=None):
        if has_in:
            for d in range(2):
                move_copy(k - LAG, d).wait_recv()
        if has_own or has_in == 1:
            slot = mod(k, SEND_SLOTS)
            for d in range(2):
                if reuse_send:
                    move_copy(k - SEND_SLOTS, d).wait_send()
                if has_own:
                    rows = pl.ds(piece_row(k, d), PIECE)
                    held = [[wall[l, q, rows, :] for q in range(4)] for l in range(LAYERS)]
                for m, (l, s_loc, is_src, _, _, _) in enumerate(info):
                    if has_own:
                        v = pick(held[l], s_loc)
                        if has_in:
                            v = jnp.where(is_src, v, mrecv[d, mod(k - LAG, RECV_SLOTS), m])
                    else:
                        v = mrecv[d, mod(k - LAG, RECV_SLOTS), m]
                    msend[d, slot, m] = v
                move_copy(k, d).start()
        if emits:
            emit(k - 3 * LAG, reuse_out, (k - 3 * LAG) // per_phase if ph is None else ph)

    first_full = 3 * LAG + OUT_SLOTS

    def one_step(k):
        if k < n_step:
            step(k, k < n_piece, 1 if k >= LAG else 0, k >= SEND_SLOTS, k >= 3 * LAG, k >= first_full)
        else:
            step(k, False, 2, False, k >= 3 * LAG, k >= first_full)

    cursor = [0]

    def moves(count):
        a = cursor[0]
        b = min(a + count, n_step + LAG)
        cursor[0] = b
        k = a
        while k < b and k < first_full:
            one_step(k)
            k += 1
        while k < min(b, n_piece):
            ph = (k - 3 * LAG) // per_phase
            mid = min(b, n_piece, 3 * LAG + (ph + 1) * per_phase)

            def loop_body(kk, carry, ph=ph):
                step(kk, True, 1, True, True, True, ph)
                return carry

            lax.fori_loop(k, mid, loop_body, 0)
            k = mid
        while k < b:
            one_step(k)
            k += 1

    def unit(l, u, per_slot=0):
        def one(q):
            outs = swiglu(tbuf[l, u], wall.at[l, q])
            col = gates(l, u, q)
            for j in range(2):
                cols = pl.ds(j * d_ff, d_ff)
                pbuf[u, :, cols] = pbuf[u, :, cols] + col * outs[j]

        if u == 0:
            x = tbuf[l, 0]
            outs = swiglu(x, shw.at[l])
            for j in range(2):
                pbuf[0, :, j * d_ff:(j + 1) * d_ff] = x[:, j * d_ff:(j + 1) * d_ff].astype(f32) + outs[j]
        else:
            pbuf[u] = jnp.zeros(pbuf.shape[1:], f32)
        first = cursor[0]
        end = first + 4 * per_slot
        ph = (first - 3 * LAG) // per_phase
        if per_slot and first_full <= first and end <= min(n_piece, 3 * LAG + (ph + 1) * per_phase):
            cursor[0] = end

            def body(q, carry):
                one(q)
                for r in range(per_slot):
                    step(first + q * per_slot + r, True, 1, True, True, True, ph)
                return carry

            lax.fori_loop(0, 4, body, 0)
        elif per_slot:
            for q in range(4):
                one(q)
                moves(per_slot)
        else:
            def plain(q, carry):
                one(q)
                return carry

            lax.fori_loop(0, 4, plain, 0)

    for l in range(LAYERS):
        for c in range(CHUNKS):
            for cp in ag_copies(l, c, tbuf.at[l, 0], (0, 2)):
                cp.wait_recv()
            relay(l, c, 0).start()
            relay(l, c, 1).start()
            moves(PLACE['relay'][l])
        if l == 0:
            for c in own_load(0):
                c.wait()
            for c in partner_load(0):
                c.wait_recv()
            for c in coefs:
                c.wait_recv()
        lo, hi = pl.ds(0, half), pl.ds(half, half)

        def pure(ll):
            return [rdma(pbuf.at[1, lo, :], rpure.at[ll, lo, :], pu_send.at[ll, 0], pu_recv.at[ll, 0], dev_l),
                    rdma(pbuf.at[1, hi, :], rpure.at[ll, hi, :], pu_send.at[ll, 1], pu_recv.at[ll, 1], dev_r)]

        def opp(ll, c):
            a, b = pl.ds(c * ch, ch), pl.ds(half + c * ch, ch)
            return [rdma(pbuf.at[3, a, :], ropp.at[ll, b, :], op_send.at[ll, 0, c], op_recv.at[ll, 0, c], dev_r),
                    rdma(pbuf.at[3, b, :], ropp.at[ll, a, :], op_send.at[ll, 1, c], op_recv.at[ll, 1, c], dev_l)]

        def summed(ll, c):
            a, b = pl.ds(c * ch, ch), pl.ds(half + c * ch, ch)
            return [rdma(pbuf.at[2, a, :], rsum.at[ll, b, :], sm_send.at[ll, 0, c], sm_recv.at[ll, 0, c], dev_l),
                    rdma(pbuf.at[2, b, :], rsum.at[ll, a, :], sm_send.at[ll, 1, c], sm_recv.at[ll, 1, c], dev_r)]

        if l > 0:
            for cp in pure(l - 1):
                cp.wait_send()
        unit(l, 1)
        moves(PLACE['u1'][l])
        for cp in pure(l):
            cp.start()
        if l == 0:
            for c in own_load(1):
                c.wait()
            for c in partner_load(1):
                c.wait_recv()
        for c in range(CHUNKS):
            for cp in ag_copies(l, c, tbuf.at[l, 0], (1, 3)):
                cp.wait_recv()
            if l > 0:
                for cp in summed(l - 1, c):
                    cp.wait_send()
        unit(l, 2)
        moves(PLACE['u2'][l])
        for c in range(CHUNKS):
            relay(l, c, 0).wait_recv()
            relay(l, c, 1).wait_recv()
            if l > 0:
                for cp in opp(l - 1, c):
                    cp.wait_send()
        unit(l, 3)
        for c in range(CHUNKS):
            for cp in opp(l, c):
                cp.start()
        moves(PLACE['u3'][l])
        if l == 0:
            tok_load.wait()
        for c in shared_load(l):
            c.wait()
        unit(l, 0)
        moves(PLACE['own'][l])
        for c in range(CHUNKS):
            a, b = pl.ds(c * ch, ch), pl.ds(half + c * ch, ch)
            for cp in opp(l, c):
                cp.wait_recv()
            for rows in (a, b):
                pbuf[2, rows, :] = pbuf[2, rows, :] + ropp[l, rows, :]
            for cp in summed(l, c):
                cp.start()
            moves(PLACE['sum'][l])
        for cp in pure(l):
            cp.wait_recv()
        for c in range(CHUNKS):
            a, b = pl.ds(c * ch, ch), pl.ds(half + c * ch, ch)
            for cp in summed(l, c):
                cp.wait_recv()
            for rows in (a, b):
                new = (pbuf[0, rows, :] + rpure[l, rows, :] + rsum[l, rows, :]).astype(bf16)
                if l + 1 < LAYERS:
                    tbuf[l + 1, 0, rows, :] = new
                else:
                    tok_out[rows, :] = new
            if l + 1 < LAYERS:
                ag_start(l + 1, tbuf.at[l + 1, 0], [c], (0, 1, 2, 3))
            moves(PLACE['fin'][l])

    moves(n_step + LAG)

    for k in range(n_step - SEND_SLOTS, n_step):
        for d in range(2):
            move_copy(k, d).wait_send()
    for i in range(n_piece - OUT_SLOTS, n_piece):
        for d in range(2):
            own, far = out_copies(i, d)
            own.wait()
            far.wait_send()
    for ph in range(3):
        arrived = (og, ou)[ph].at[:, :, pl.ds(0, 2 * quarter), :] if ph < 2 else od.at[:, :, :, pl.ds(0, d_ff)]
        pltpu.make_async_copy(arrived, arrived, mo_recv.at[ph]).wait()
    last = LAYERS - 1
    for cp in pure(last):
        cp.wait_send()
    for c in range(CHUNKS):
        for cp in opp(last, c) + summed(last, c):
            cp.wait_send()
    for l in range(LAYERS):
        for c in range(CHUNKS):
            for cp in ag_copies(l, c, tok if l == 0 else tbuf.at[l, 0], (0, 1, 2, 3)):
                cp.wait_send()
            relay(l, c, 0).wait_send()
            relay(l, c, 1).wait_send()
        for cp in partner_load(l):
            cp.wait_send()
    for cp in coefs:
        cp.wait_send()


def fused(n_ep, old_map, move_slot, move_expert, routes, gate_vals, tok, wg, wu, wd, sg, su, sd):
    toks, d_model = tok.shape
    d_ff = sg.shape[-1]
    n_chip = n_ep // 2
    rows = 3 * d_model
    f32, bf16 = jnp.float32, jnp.bfloat16
    any_spec = pl.BlockSpec(memory_space=pl.ANY)
    vmem = pl.BlockSpec(memory_space=pltpu.VMEM)
    smem = pl.BlockSpec(memory_space=pltpu.SMEM)
    dma = pltpu.SemaphoreType.DMA
    return pl.pallas_call(
        functools.partial(kernel, n_chip, (toks, d_model, d_ff)),
        out_shape=(jax.ShapeDtypeStruct((toks, d_model), bf16),) + tuple(jax.ShapeDtypeStruct(w.shape, bf16) for w in (wg, wu, wd)),
        in_specs=[smem] * 3 + [vmem] * 2 + [any_spec] * 7,
        out_specs=(vmem, any_spec, any_spec, any_spec),
        scratch_shapes=[
            pltpu.VMEM((LAYERS, 4, rows, d_ff), bf16),
            pltpu.VMEM((LAYERS, rows, d_ff), bf16),
            pltpu.VMEM((LAYERS, 4, toks, d_model), bf16),
            pltpu.VMEM((4, toks, d_model), f32),
            pltpu.VMEM((LAYERS, toks, d_model), f32),
            pltpu.VMEM((LAYERS, toks, d_model), f32),
            pltpu.VMEM((LAYERS, toks, d_model), f32),
            pltpu.VMEM((n_chip, LAYERS * 4, 1, toks), f32),
            pltpu.VMEM((3, LAYERS * 4, 1, toks), f32),
            pltpu.VMEM((2, RECV_SLOTS, 4, PIECE, d_ff), bf16),
            pltpu.VMEM((2, SEND_SLOTS, 4, PIECE, d_ff), bf16),
            pltpu.VMEM((OUT_SLOTS, 2, 2, LAYERS, 2, PIECE, d_ff), bf16),
            dma((LAYERS, 4)), dma((LAYERS, 4)), dma((LAYERS, 4)), dma((LAYERS, 4)), dma(()), dma((3,)), dma((3,)),
            dma((LAYERS, 4, CHUNKS)), dma((LAYERS, 4, CHUNKS)), dma((LAYERS, 2, CHUNKS)), dma((LAYERS, 2, CHUNKS)),
            dma((LAYERS, 2)), dma((LAYERS, 2)),
            dma((LAYERS, 2, CHUNKS)), dma((LAYERS, 2, CHUNKS)), dma((LAYERS, 2, CHUNKS)), dma((LAYERS, 2, CHUNKS)),
            dma((2, SEND_SLOTS)), dma((2, RECV_SEMS)), dma((OUT_SLOTS, 2)), dma((OUT_SLOTS, 2)), dma((3,)),
        ],
        compiler_params=pltpu.CompilerParams(collective_id=0, has_side_effects=True, vmem_limit_bytes=67043328),
    )(old_map, move_slot, move_expert, routes, gate_vals, tok, wg, wu, wd, sg, su, sd)


def solution(mesh):
    n_ep = mesh.shape['ep']

    def body(tok_in, routes, gate_vals, w_gate, w_up, w_down, sh_gate, sh_up, sh_down, old_map, move_slot, move_expert):
        return fused(n_ep, old_map, move_slot, move_expert, routes.transpose(0, 2, 1), gate_vals.transpose(0, 2, 1),
                     tok_in, w_gate, w_up, w_down, sh_gate, sh_up, sh_down)

    weight_spec = P(None, TOKEN_AXES, None, None)
    route_spec = P(None, TOKEN_AXES, None)
    map_spec = P(None, 'replica')
    shared_spec = P(None, None, None)
    tok_spec = P(TOKEN_AXES, None)
    return jax.shard_map(body, mesh=mesh, in_specs=(tok_spec, route_spec, route_spec, weight_spec, weight_spec, weight_spec, shared_spec, shared_spec, shared_spec, map_spec, map_spec, map_spec), out_specs=(tok_spec, weight_spec, weight_spec, weight_spec), check_vma=False)
```

```python
import functools

import jax
import jax.numpy as jnp
from jax import lax
from jax.experimental import pallas as pl
from jax.experimental.pallas import tpu as pltpu
from jax.sharding import PartitionSpec as P

TOKEN_AXES = ('replica', 'ep')
MESH = pl.DeviceIdType.MESH
CHUNKS = 4
PIECE = 16
LAG = 4
SEND_SLOTS = LAG + 2
OUT_SLOTS = 4
RECV_SEMS = 4 * LAG
RECV_SLOTS = 6 * LAG + 2
LAYERS = 2
VMEM_LIMIT = 46 * 2 ** 20
PLACE = {'relay': (0, 0), 'u1': (0, 4), 'u2': (0, 4), 'u3': (2, 4), 'own': (4, 4), 'sum': (2, 2), 'fin': (2, 1)}


def kernel(n_chip, dims, old_map, move_slot, move_expert, routes, gate_vals, tok, wg, wu, wd, sg, su, sd,
           tok_out, og, ou, od,
           wall, shw, tbuf, pbuf, rpure, ropp, rsum, coef, crecv, mrecv, msend, mout,
           own_sem, w_send, w_recv, sh_sem, tok_sem, c_send, c_recv,
           ag_send, ag_recv, rl_send, rl_recv, pu_send, pu_recv,
           op_send, op_recv, sm_send, sm_recv,
           mv_send, mv_recv, mo_send, mo_recv):
    toks, d_model, d_ff = dims
    half = toks // 2
    ch = half // CHUNKS
    quarter = d_model // 4
    per_phase = quarter // PIECE
    n_piece = 3 * per_phase
    n_step = n_piece + 2 * LAG
    f32, bf16 = jnp.float32, jnp.bfloat16

    me = lax.axis_index('ep')
    chip = me // 2
    core = lax.rem(me, 2)
    dev_r = lax.rem(chip + 1, n_chip) * 2 + core
    dev_l = lax.rem(chip + n_chip - 1, n_chip) * 2 + core
    dev_o = lax.rem(chip + 2, n_chip) * 2 + core
    dev_p = chip * 2 + 1 - core

    def rdma(src, dst, ss, rs, dev):
        return pltpu.make_async_remote_copy(src_ref=src, dst_ref=dst, send_sem=ss, recv_sem=rs,
                                            device_id={'ep': dev}, device_id_type=MESH)

    base = core * 2
    mine = pl.ds(base, 2)
    loads = []

    def weight_parts(l, g, u, d):
        return [(g, pl.ds(0, d_model), None), (u, pl.ds(d_model, d_model), None),
                (d, pl.ds(2 * d_model, d_ff), 0), (d, pl.ds(2 * d_model + d_ff, d_ff), 1)]

    def src_of(ref, col, l):
        if col is None:
            return ref.at[l]
        cols = pl.ds(col * d_ff, d_ff)
        return ref.at[l, :, :, cols] if len(ref.shape) == 4 else ref.at[l, :, cols]

    def own_load(l):
        return [pltpu.make_async_copy(src_of(r, c, l), wall.at[l, mine, rows, :], own_sem.at[l, i])
                for i, (r, rows, c) in enumerate(weight_parts(l, wg, wu, wd))]

    def shared_load(l):
        return [pltpu.make_async_copy(src_of(r, c, l), shw.at[rows, :], sh_sem.at[l, i])
                for i, (r, rows, c) in enumerate(weight_parts(l, sg, su, sd))]

    def partner_load(l):
        return [rdma(src_of(r, c, l), wall.at[l, mine, rows, :], w_send.at[l, i], w_recv.at[l, i], dev_p)
                for i, (r, rows, c) in enumerate(weight_parts(l, wg, wu, wd))]

    tok_load = pltpu.make_async_copy(tok, tbuf.at[0, 0], tok_sem)
    tok_load.start()
    for c in own_load(0):
        c.start()

    n_slot = n_chip * 4
    for l in range(LAYERS):
        ids = [old_map[l, q] for q in range(n_slot)]
        for q in range(n_slot):
            want = ids[q]
            for p in range(q):
                want = jnp.where(ids[p] == ids[q], -1, want)
            row = jnp.sum(jnp.where(routes[l] == want, gate_vals[l], 0.0), axis=0, keepdims=True)
            coef[q // 4, l * 4 + q % 4] = row

    barrier = pltpu.get_barrier_semaphore()
    for dev in (dev_l, dev_r, dev_o, dev_p):
        pl.semaphore_signal(barrier, inc=1, device_id={'ep': dev}, device_id_type=MESH)
    pl.semaphore_wait(barrier, 4)

    def ag_copies(l, c, src, kinds):
        lo, hi = pl.ds(c * ch, ch), pl.ds(half + c * ch, ch)
        form = [(lo, 1, lo, dev_r), (hi, 2, lo, dev_r), (hi, 1, hi, dev_l), (lo, 2, hi, dev_l)]
        return [rdma(src.at[form[k][0], :], tbuf.at[l, form[k][1], form[k][2], :],
                     ag_send.at[l, k, c], ag_recv.at[l, k, c], form[k][3]) for k in kinds]

    def ag_start(l, src, c_list, kinds):
        for c in c_list:
            for cp in ag_copies(l, c, src, kinds):
                cp.start()

    def relay(l, c, side):
        rows = pl.ds(c * ch, ch) if side == 0 else pl.ds(half + c * ch, ch)
        dev = dev_r if side == 0 else dev_l
        return rdma(tbuf.at[l, 1, rows, :], tbuf.at[l, 3, rows, :], rl_send.at[l, side, c], rl_recv.at[l, side, c], dev)

    ag_start(0, tok, range(CHUNKS), (0, 2))
    cl = lax.rem(chip + n_chip - 1, n_chip)
    cr = lax.rem(chip + 1, n_chip)
    co = lax.rem(chip + 2, n_chip)
    coefs = [rdma(coef.at[cr], crecv.at[0], c_send.at[0], c_recv.at[0], dev_r),
             rdma(coef.at[cl], crecv.at[1], c_send.at[1], c_recv.at[1], dev_l),
             rdma(coef.at[co], crecv.at[2], c_send.at[2], c_recv.at[2], dev_o)]
    for c in coefs:
        c.start()
    for c in partner_load(0):
        c.start()
    ag_start(0, tok, range(CHUNKS), (1, 3))
    for c in shared_load(0) + own_load(1):
        c.start()
    for c in partner_load(1):
        c.start()

    eye = lax.broadcasted_iota(jnp.int32, (half, half), 0) == lax.broadcasted_iota(jnp.int32, (half, half), 1)

    def column(row):
        return jnp.sum(jnp.where(eye, jnp.broadcast_to(row, (half, half)), 0.0), axis=1, keepdims=True)

    def gates(l, u, q):
        s = l * 4 + q
        lo, hi = pl.ds(0, half), pl.ds(half, half)
        if u == 0:
            a, b = coef[chip, s, :, lo], coef[chip, s, :, hi]
        elif u == 1:
            a, b = crecv[0, s, :, lo], crecv[1, s, :, hi]
        elif u == 2:
            a, b = crecv[0, s, :, hi], crecv[1, s, :, lo]
        else:
            a, b = crecv[2, s, :, lo], crecv[2, s, :, hi]
        return jnp.concatenate([column(a), column(b)], axis=0)

    def swiglu(x, w):
        g = jnp.dot(x, w[pl.ds(0, d_model), :], preferred_element_type=f32)
        u = jnp.dot(x, w[pl.ds(d_model, d_model), :], preferred_element_type=f32)
        inner = (jax.nn.silu(g) * u).astype(bf16)
        return [jnp.dot(inner, w[pl.ds(2 * d_model + j * d_ff, d_ff), :], preferred_element_type=f32) for j in range(2)]

    info = []
    for m in range(2 * LAYERS):
        t, want = move_slot[m // 2, m % 2], move_expert[m // 2, m % 2]
        s = jnp.int32(0)
        for q in range(n_slot - 1, 0, -1):
            s = jnp.where(old_map[m // 2, q] == want, q, s)
        s_chip, s_loc = s >> 2, s & 3
        t_chip, t_loc = t >> 2, t & 3
        dist = [(t_chip - s_chip) & (n_chip - 1), (s_chip - t_chip) & (n_chip - 1)]
        info.append((m // 2, s_loc, s_chip == chip, dist, t_chip == chip, t_loc))

    def piece_row(i, d):
        if isinstance(i, int):
            ph, rest = i // per_phase, i % per_phase
        else:
            ph, rest = lax.div(i, per_phase), lax.rem(i, per_phase)
        return pl.multiple_of(ph * d_model + core * 2 * quarter + d * quarter + rest * PIECE, PIECE)

    def mod(k, n):
        return k % n if isinstance(k, int) else lax.rem(k, n)

    def move_copy(k, d):
        slot = mod(k, SEND_SLOTS)
        return rdma(msend.at[d, slot], mrecv.at[d, mod(k, RECV_SLOTS)], mv_send.at[d, slot], mv_recv.at[d, mod(k, RECV_SEMS)],
                    dev_r if d == 0 else dev_l)

    def place(ph, rest, d):
        row = pl.multiple_of(d * quarter + rest * PIECE, PIECE)
        if ph < 2:
            return (og, ou)[ph], pl.ds(pl.multiple_of(row + core * 2 * quarter, PIECE), PIECE), pl.ds(0, d_ff)
        return od, pl.ds(row, PIECE), pl.ds(pl.multiple_of(core * d_ff, d_ff), d_ff)

    def far_copy(i, d, ph=0):
        slot = mod(i, OUT_SLOTS)
        ref, rows, cols = place(ph, mod(i, per_phase), d)
        return rdma(mout.at[slot, d], ref.at[:, :, rows, cols], mo_send.at[slot, d], mo_recv.at[ph], dev_p)

    def pick(options, which):
        v = options[0]
        for q in range(1, 4):
            v = jnp.where(which == q, options[q], v)
        return v

    def emit(i, reuse, ph):
        slot = mod(i, OUT_SLOTS)
        for d in range(2):
            if reuse:
                far_copy(i - OUT_SLOTS, d).wait_send()
            rows = pl.ds(piece_row(i, d), PIECE)
            held = [[wall[l, q, rows, :] for q in range(4)] for l in range(LAYERS)]
            near = [[wall[l, base + j, rows, :] for j in range(2)] for l in range(LAYERS)]
            away = [[wall[l, 2 - base + j, rows, :] for j in range(2)] for l in range(LAYERS)]
            vals = []
            for m, (l, s_loc, _, dist, _, _) in enumerate(info):
                h = dist[d]
                v = pick(held[l], s_loc)
                for j in range(3):
                    v = jnp.where(h == j + 1, mrecv[d, mod(i + j * LAG, RECV_SLOTS), m], v)
                vals.append(v)
            for which in range(2):
                for j in range(2):
                    q = base + j if which == 0 else 2 - base + j
                    for l in range(LAYERS):
                        v = (away if which else near)[l][j]
                        for m in (2 * l, 2 * l + 1):
                            hit = jnp.logical_and(info[m][4], info[m][5] == q)
                            v = jnp.where(hit, vals[m], v)
                        if which:
                            mout[slot, d, l, j] = v
                        else:
                            ref, to_rows, to_cols = place(ph, mod(i, per_phase), d)
                            ref[l, j, to_rows, to_cols] = v
            far_copy(i, d, ph).start()

    def step(k, has_own, has_in, reuse_send, emits, reuse_out, ph=None):
        if has_in:
            for d in range(2):
                move_copy(k - LAG, d).wait_recv()
        if has_own or has_in == 1:
            slot = mod(k, SEND_SLOTS)
            for d in range(2):
                if reuse_send:
                    move_copy(k - SEND_SLOTS, d).wait_send()
                if has_own:
                    rows = pl.ds(piece_row(k, d), PIECE)
                    held = [[wall[l, q, rows, :] for q in range(4)] for l in range(LAYERS)]
                for m, (l, s_loc, is_src, _, _, _) in enumerate(info):
                    if has_own:
                        v = pick(held[l], s_loc)
                        if has_in:
                            v = jnp.where(is_src, v, mrecv[d, mod(k - LAG, RECV_SLOTS), m])
                    else:
                        v = mrecv[d, mod(k - LAG, RECV_SLOTS), m]
                    msend[d, slot, m] = v
                move_copy(k, d).start()
        if emits:
            emit(k - 3 * LAG, reuse_out, (k - 3 * LAG) // per_phase if ph is None else ph)

    first_full = 3 * LAG + OUT_SLOTS

    def one_step(k):
        if k < n_step:
            step(k, k < n_piece, 1 if k >= LAG else 0, k >= SEND_SLOTS, k >= 3 * LAG, k >= first_full)
        else:
            step(k, False, 2, False, k >= 3 * LAG, k >= first_full)

    cursor = [0]

    def moves(count):
        a = cursor[0]
        b = min(a + count, n_step + LAG)
        cursor[0] = b
        k = a
        while k < b and k < first_full:
            one_step(k)
            k += 1
        while k < min(b, n_piece):
            ph = (k - 3 * LAG) // per_phase
            mid = min(b, n_piece, 3 * LAG + (ph + 1) * per_phase)

            def loop_body(kk, carry, ph=ph):
                step(kk, True, 1, True, True, True, ph)
                return carry

            lax.fori_loop(k, mid, loop_body, 0)
            k = mid
        while k < b:
            one_step(k)
            k += 1

    def unit(l, u, per_slot=0):
        def one(q):
            outs = swiglu(tbuf[l, u], wall.at[l, q])
            col = gates(l, u, q)
            for j in range(2):
                cols = pl.ds(j * d_ff, d_ff)
                pbuf[u, :, cols] = pbuf[u, :, cols] + col * outs[j]

        if u == 0:
            x = tbuf[l, 0]
            outs = swiglu(x, shw)
            for j in range(2):
                pbuf[0, :, j * d_ff:(j + 1) * d_ff] = x[:, j * d_ff:(j + 1) * d_ff].astype(f32) + outs[j]
        else:
            pbuf[u] = jnp.zeros(pbuf.shape[1:], f32)
        first = cursor[0]
        end = first + 4 * per_slot
        ph = (first - 3 * LAG) // per_phase
        if per_slot and first_full <= first and end <= min(n_piece, 3 * LAG + (ph + 1) * per_phase):
            cursor[0] = end

            def body(q, carry):
                one(q)
                for r in range(per_slot):
                    step(first + q * per_slot + r, True, 1, True, True, True, ph)
                return carry

            lax.fori_loop(0, 4, body, 0)
        elif per_slot:
            for q in range(4):
                one(q)
                moves(per_slot)
        else:
            def plain(q, carry):
                one(q)
                return carry

            lax.fori_loop(0, 4, plain, 0)

    for l in range(LAYERS):
        for c in range(CHUNKS):
            for cp in ag_copies(l, c, tbuf.at[l, 0], (0, 2)):
                cp.wait_recv()
            relay(l, c, 0).start()
            relay(l, c, 1).start()
            moves(PLACE['relay'][l])
        if l == 0:
            for c in own_load(0):
                c.wait()
            for c in partner_load(0):
                c.wait_recv()
            for c in coefs:
                c.wait_recv()
        lo, hi = pl.ds(0, half), pl.ds(half, half)

        def pure(ll):
            return [rdma(pbuf.at[1, lo, :], rpure.at[lo, :], pu_send.at[ll, 0], pu_recv.at[ll, 0], dev_l),
                    rdma(pbuf.at[1, hi, :], rpure.at[hi, :], pu_send.at[ll, 1], pu_recv.at[ll, 1], dev_r)]

        def opp(ll, c):
            a, b = pl.ds(c * ch, ch), pl.ds(half + c * ch, ch)
            return [rdma(pbuf.at[3, a, :], ropp.at[b, :], op_send.at[ll, 0, c], op_recv.at[ll, 0, c], dev_r),
                    rdma(pbuf.at[3, b, :], ropp.at[a, :], op_send.at[ll, 1, c], op_recv.at[ll, 1, c], dev_l)]

        def summed(ll, c):
            a, b = pl.ds(c * ch, ch), pl.ds(half + c * ch, ch)
            return [rdma(pbuf.at[2, a, :], rsum.at[b, :], sm_send.at[ll, 0, c], sm_recv.at[ll, 0, c], dev_l),
                    rdma(pbuf.at[2, b, :], rsum.at[a, :], sm_send.at[ll, 1, c], sm_recv.at[ll, 1, c], dev_r)]

        if l > 0:
            for cp in pure(l - 1):
                cp.wait_send()
        unit(l, 1)
        moves(PLACE['u1'][l])
        for cp in pure(l):
            cp.start()
        if l == 0:
            for c in own_load(1):
                c.wait()
            for c in partner_load(1):
                c.wait_recv()
        for c in range(CHUNKS):
            for cp in ag_copies(l, c, tbuf.at[l, 0], (1, 3)):
                cp.wait_recv()
            if l > 0:
                for cp in summed(l - 1, c):
                    cp.wait_send()
        unit(l, 2)
        moves(PLACE['u2'][l])
        for c in range(CHUNKS):
            relay(l, c, 0).wait_recv()
            relay(l, c, 1).wait_recv()
            if l > 0:
                for cp in opp(l - 1, c):
                    cp.wait_send()
        unit(l, 3)
        for c in range(CHUNKS):
            for cp in opp(l, c):
                cp.start()
        moves(PLACE['u3'][l])
        if l == 0:
            tok_load.wait()
        for c in shared_load(l):
            c.wait()
        unit(l, 0)
        if l + 1 < LAYERS:
            for c in shared_load(l + 1):
                c.start()
        moves(PLACE['own'][l])
        for c in range(CHUNKS):
            a, b = pl.ds(c * ch, ch), pl.ds(half + c * ch, ch)
            for cp in opp(l, c):
                cp.wait_recv()
            for rows in (a, b):
                pbuf[2, rows, :] = pbuf[2, rows, :] + ropp[rows, :]
            for cp in summed(l, c):
                cp.start()
            moves(PLACE['sum'][l])
        for cp in pure(l):
            cp.wait_recv()
        for c in range(CHUNKS):
            a, b = pl.ds(c * ch, ch), pl.ds(half + c * ch, ch)
            for cp in summed(l, c):
                cp.wait_recv()
            for rows in (a, b):
                new = (pbuf[0, rows, :] + rpure[rows, :] + rsum[rows, :]).astype(bf16)
                if l + 1 < LAYERS:
                    tbuf[l + 1, 0, rows, :] = new
                else:
                    tok_out[rows, :] = new
            if l + 1 < LAYERS:
                ag_start(l + 1, tbuf.at[l + 1, 0], [c], (0, 1, 2, 3))
            moves(PLACE['fin'][l])

    moves(n_step + LAG)

    for k in range(n_step - SEND_SLOTS, n_step):
        for d in range(2):
            move_copy(k, d).wait_send()
    for i in range(n_piece - OUT_SLOTS, n_piece):
        for d in range(2):
            far_copy(i, d).wait_send()
    for ph in range(3):
        arrived = (og, ou)[ph].at[:, :, pl.ds(0, 2 * quarter), :] if ph < 2 else od.at[:, :, :, pl.ds(0, d_ff)]
        pltpu.make_async_copy(arrived, arrived, mo_recv.at[ph]).wait()
    last = LAYERS - 1
    for cp in pure(last):
        cp.wait_send()
    for c in range(CHUNKS):
        for cp in opp(last, c) + summed(last, c):
            cp.wait_send()
    for l in range(LAYERS):
        for c in range(CHUNKS):
            for cp in ag_copies(l, c, tok if l == 0 else tbuf.at[l, 0], (0, 1, 2, 3)):
                cp.wait_send()
            relay(l, c, 0).wait_send()
            relay(l, c, 1).wait_send()
        for cp in partner_load(l):
            cp.wait_send()
    for cp in coefs:
        cp.wait_send()


def fused(n_ep, old_map, move_slot, move_expert, routes, gate_vals, tok, wg, wu, wd, sg, su, sd):
    toks, d_model = tok.shape
    d_ff = sg.shape[-1]
    n_chip = n_ep // 2
    rows = 3 * d_model
    f32, bf16 = jnp.float32, jnp.bfloat16
    hbm = pl.BlockSpec(memory_space=pltpu.HBM)
    vmem = pl.BlockSpec(memory_space=pltpu.VMEM)
    smem = pl.BlockSpec(memory_space=pltpu.SMEM)
    dma = pltpu.SemaphoreType.DMA
    return pl.pallas_call(
        functools.partial(kernel, n_chip, (toks, d_model, d_ff)),
        out_shape=(jax.ShapeDtypeStruct((toks, d_model), bf16),) + tuple(pltpu.VMEM(w.shape, bf16) for w in (wg, wu, wd)),
        in_specs=[smem] * 3 + [vmem] * 2 + [hbm] * 7,
        out_specs=(vmem, vmem, vmem, vmem),
        scratch_shapes=[
            pltpu.VMEM((LAYERS, 4, rows, d_ff), bf16),
            pltpu.VMEM((rows, d_ff), bf16),
            pltpu.VMEM((LAYERS, 4, toks, d_model), bf16),
            pltpu.VMEM((4, toks, d_model), f32),
            pltpu.VMEM((toks, d_model), f32),
            pltpu.VMEM((toks, d_model), f32),
            pltpu.VMEM((toks, d_model), f32),
            pltpu.VMEM((n_chip, LAYERS * 4, 1, toks), f32),
            pltpu.VMEM((3, LAYERS * 4, 1, toks), f32),
            pltpu.VMEM((2, RECV_SLOTS, 4, PIECE, d_ff), bf16),
            pltpu.VMEM((2, SEND_SLOTS, 4, PIECE, d_ff), bf16),
            pltpu.VMEM((OUT_SLOTS, 2, LAYERS, 2, PIECE, d_ff), bf16),
            dma((LAYERS, 4)), dma((LAYERS, 4)), dma((LAYERS, 4)), dma((LAYERS, 4)), dma(()), dma((3,)), dma((3,)),
            dma((LAYERS, 4, CHUNKS)), dma((LAYERS, 4, CHUNKS)), dma((LAYERS, 2, CHUNKS)), dma((LAYERS, 2, CHUNKS)),
            dma((LAYERS, 2)), dma((LAYERS, 2)),
            dma((LAYERS, 2, CHUNKS)), dma((LAYERS, 2, CHUNKS)), dma((LAYERS, 2, CHUNKS)), dma((LAYERS, 2, CHUNKS)),
            dma((2, SEND_SLOTS)), dma((2, RECV_SEMS)), dma((OUT_SLOTS, 2)), dma((3,)),
        ],
        compiler_params=pltpu.CompilerParams(collective_id=0, has_side_effects=True, vmem_limit_bytes=VMEM_LIMIT),
    )(old_map, move_slot, move_expert, routes, gate_vals, tok, wg, wu, wd, sg, su, sd)


def solution(mesh):
    n_ep = mesh.shape['ep']

    def body(tok_in, routes, gate_vals, w_gate, w_up, w_down, sh_gate, sh_up, sh_down, old_map, move_slot, move_expert):
        return fused(n_ep, old_map, move_slot, move_expert, routes.transpose(0, 2, 1), gate_vals.transpose(0, 2, 1),
                     tok_in, w_gate, w_up, w_down, sh_gate, sh_up, sh_down)

    weight_spec = P(None, TOKEN_AXES, None, None)
    route_spec = P(None, TOKEN_AXES, None)
    map_spec = P(None, 'replica')
    shared_spec = P(None, None, None)
    tok_spec = P(TOKEN_AXES, None)
    return jax.shard_map(body, mesh=mesh, in_specs=(tok_spec, route_spec, route_spec, weight_spec, weight_spec, weight_spec, shared_spec, shared_spec, shared_spec, map_spec, map_spec, map_spec), out_specs=(tok_spec, weight_spec, weight_spec, weight_spec), check_vma=False)
```

```python
import functools

import jax
import jax.numpy as jnp
from jax import lax
from jax.experimental import pallas as pl
from jax.experimental.pallas import tpu as pltpu
from jax.sharding import PartitionSpec as P

TOKEN_AXES = ('replica', 'ep')
MESH = pl.DeviceIdType.MESH
CHUNKS = 4
PIECE = 16
LAG = 4
SEND_SLOTS = LAG + 2
OUT_SLOTS = 4
RECV_SEMS = 4 * LAG
RECV_SLOTS = 6 * LAG + 2
LAYERS = 2
VMEM_LIMIT = 46 * 2 ** 20
PLACE = {'relay': (0, 0), 'u1': (0, 4), 'u2': (0, 4), 'u3': (2, 4), 'own': (4, 4), 'sum': (2, 2), 'fin': (2, 1)}


def kernel(n_chip, dims, old_map, move_slot, move_expert, routes, gate_vals, tok, wg, wu, wd, sg, su, sd,
           tok_out, og, ou, od,
           wall, shw, tbuf, pbuf, rpure, ropp, rsum, coef, crecv, mrecv, msend, mout,
           own_sem, w_send, w_recv, sh_sem, tok_sem, c_send, c_recv,
           ag_send, ag_recv, rl_send, rl_recv, pu_send, pu_recv,
           op_send, op_recv, sm_send, sm_recv,
           mv_send, mv_recv, mo_send, mo_recv):
    toks, d_model, d_ff = dims
    half = toks // 2
    ch = half // CHUNKS
    quarter = d_model // 4
    per_phase = quarter // PIECE
    n_piece = 3 * per_phase
    n_step = n_piece + 2 * LAG
    f32, bf16 = jnp.float32, jnp.bfloat16

    me = lax.axis_index('ep')
    chip = me // 2
    core = lax.rem(me, 2)
    dev_r = lax.rem(chip + 1, n_chip) * 2 + core
    dev_l = lax.rem(chip + n_chip - 1, n_chip) * 2 + core
    dev_o = lax.rem(chip + 2, n_chip) * 2 + core
    dev_p = chip * 2 + 1 - core

    def rdma(src, dst, ss, rs, dev):
        return pltpu.make_async_remote_copy(src_ref=src, dst_ref=dst, send_sem=ss, recv_sem=rs,
                                            device_id={'ep': dev}, device_id_type=MESH)

    base = core * 2
    mine = pl.ds(base, 2)
    loads = []

    def weight_parts(l, g, u, d):
        return [(g, pl.ds(0, d_model), None), (u, pl.ds(d_model, d_model), None),
                (d, pl.ds(2 * d_model, d_ff), 0), (d, pl.ds(2 * d_model + d_ff, d_ff), 1)]

    def src_of(ref, col, l):
        if col is None:
            return ref.at[l]
        cols = pl.ds(col * d_ff, d_ff)
        return ref.at[l, :, :, cols] if len(ref.shape) == 4 else ref.at[l, :, cols]

    def own_load(l):
        return [pltpu.make_async_copy(src_of(r, c, l), wall.at[l, mine, rows, :], own_sem.at[l, i])
                for i, (r, rows, c) in enumerate(weight_parts(l, wg, wu, wd))]

    def shared_load(l):
        return [pltpu.make_async_copy(src_of(r, c, l), shw.at[rows, :], sh_sem.at[l, i])
                for i, (r, rows, c) in enumerate(weight_parts(l, sg, su, sd))]

    def partner_load(l):
        return [rdma(src_of(r, c, l), wall.at[l, mine, rows, :], w_send.at[l, i], w_recv.at[l, i], dev_p)
                for i, (r, rows, c) in enumerate(weight_parts(l, wg, wu, wd))]

    tok_load = pltpu.make_async_copy(tok, tbuf.at[0, 0], tok_sem)
    tok_load.start()
    for c in own_load(0):
        c.start()

    n_slot = n_chip * 4
    for l in range(LAYERS):
        ids = [old_map[l, q] for q in range(n_slot)]
        for q in range(n_slot):
            want = ids[q]
            for p in range(q):
                want = jnp.where(ids[p] == ids[q], -1, want)
            row = jnp.sum(jnp.where(routes[l] == want, gate_vals[l], 0.0), axis=0, keepdims=True)
            coef[q // 4, l * 4 + q % 4] = row

    barrier = pltpu.get_barrier_semaphore()
    for dev in (dev_l, dev_r, dev_o, dev_p):
        pl.semaphore_signal(barrier, inc=1, device_id={'ep': dev}, device_id_type=MESH)
    pl.semaphore_wait(barrier, 4)

    def ag_copies(l, c, src, kinds):
        lo, hi = pl.ds(c * ch, ch), pl.ds(half + c * ch, ch)
        form = [(lo, 1, lo, dev_r), (hi, 2, lo, dev_r), (hi, 1, hi, dev_l), (lo, 2, hi, dev_l)]
        return [rdma(src.at[form[k][0], :], tbuf.at[l, form[k][1], form[k][2], :],
                     ag_send.at[l, k, c], ag_recv.at[l, k, c], form[k][3]) for k in kinds]

    def ag_start(l, src, c_list, kinds):
        for c in c_list:
            for cp in ag_copies(l, c, src, kinds):
                cp.start()

    def relay(l, c, side):
        rows = pl.ds(c * ch, ch) if side == 0 else pl.ds(half + c * ch, ch)
        dev = dev_r if side == 0 else dev_l
        return rdma(tbuf.at[l, 1, rows, :], tbuf.at[l, 3, rows, :], rl_send.at[l, side, c], rl_recv.at[l, side, c], dev)

    ag_start(0, tok, range(CHUNKS), (0, 2))
    cl = lax.rem(chip + n_chip - 1, n_chip)
    cr = lax.rem(chip + 1, n_chip)
    co = lax.rem(chip + 2, n_chip)
    coefs = [rdma(coef.at[cr], crecv.at[0], c_send.at[0], c_recv.at[0], dev_r),
             rdma(coef.at[cl], crecv.at[1], c_send.at[1], c_recv.at[1], dev_l),
             rdma(coef.at[co], crecv.at[2], c_send.at[2], c_recv.at[2], dev_o)]
    for c in coefs:
        c.start()
    for c in partner_load(0):
        c.start()
    ag_start(0, tok, range(CHUNKS), (1, 3))
    for c in shared_load(0) + own_load(1):
        c.start()
    for c in partner_load(1):
        c.start()

    eye = lax.broadcasted_iota(jnp.int32, (half, half), 0) == lax.broadcasted_iota(jnp.int32, (half, half), 1)

    def column(row):
        return jnp.sum(jnp.where(eye, jnp.broadcast_to(row, (half, half)), 0.0), axis=1, keepdims=True)

    def gates(l, u, q):
        s = l * 4 + q
        lo, hi = pl.ds(0, half), pl.ds(half, half)
        if u == 0:
            a, b = coef[chip, s, :, lo], coef[chip, s, :, hi]
        elif u == 1:
            a, b = crecv[0, s, :, lo], crecv[1, s, :, hi]
        elif u == 2:
            a, b = crecv[0, s, :, hi], crecv[1, s, :, lo]
        else:
            a, b = crecv[2, s, :, lo], crecv[2, s, :, hi]
        return jnp.concatenate([column(a), column(b)], axis=0)

    def swiglu(x, w):
        g = jnp.dot(x, w[pl.ds(0, d_model), :], preferred_element_type=f32)
        u = jnp.dot(x, w[pl.ds(d_model, d_model), :], preferred_element_type=f32)
        inner = (jax.nn.silu(g) * u).astype(bf16)
        return [jnp.dot(inner, w[pl.ds(2 * d_model + j * d_ff, d_ff), :], preferred_element_type=f32) for j in range(2)]

    info = []
    for m in range(2 * LAYERS):
        t, want = move_slot[m // 2, m % 2], move_expert[m // 2, m % 2]
        s = jnp.int32(0)
        for q in range(n_slot - 1, 0, -1):
            s = jnp.where(old_map[m // 2, q] == want, q, s)
        s_chip, s_loc = s >> 2, s & 3
        t_chip, t_loc = t >> 2, t & 3
        dist = [(t_chip - s_chip) & (n_chip - 1), (s_chip - t_chip) & (n_chip - 1)]
        info.append((m // 2, s_loc, s_chip == chip, dist, t_chip == chip, t_loc))

    def piece_row(i, d):
        if isinstance(i, int):
            ph, rest = i // per_phase, i % per_phase
        else:
            ph, rest = lax.div(i, per_phase), lax.rem(i, per_phase)
        return pl.multiple_of(ph * d_model + core * 2 * quarter + d * quarter + rest * PIECE, PIECE)

    def mod(k, n):
        return k % n if isinstance(k, int) else lax.rem(k, n)

    def move_copy(k, d):
        slot = mod(k, SEND_SLOTS)
        return rdma(msend.at[d, slot], mrecv.at[d, mod(k, RECV_SLOTS)], mv_send.at[d, slot], mv_recv.at[d, mod(k, RECV_SEMS)],
                    dev_r if d == 0 else dev_l)

    def place(ph, rest, d):
        row = pl.multiple_of(d * quarter + rest * PIECE, PIECE)
        if ph < 2:
            return (og, ou)[ph], pl.ds(pl.multiple_of(row + core * 2 * quarter, PIECE), PIECE), pl.ds(0, d_ff)
        return od, pl.ds(row, PIECE), pl.ds(pl.multiple_of(core * d_ff, d_ff), d_ff)

    def far_copy(i, d, ph=0):
        slot = mod(i, OUT_SLOTS)
        ref, rows, cols = place(ph, mod(i, per_phase), d)
        return rdma(mout.at[slot, d], ref.at[:, :, rows, cols], mo_send.at[slot, d], mo_recv.at[ph], dev_p)

    def pick(options, which):
        v = options[0]
        for q in range(1, 4):
            v = jnp.where(which == q, options[q], v)
        return v

    def emit(i, reuse, ph):
        slot = mod(i, OUT_SLOTS)
        for d in range(2):
            if reuse:
                far_copy(i - OUT_SLOTS, d).wait_send()
            rows = pl.ds(piece_row(i, d), PIECE)
            held = [[wall[l, q, rows, :] for q in range(4)] for l in range(LAYERS)]
            near = [[wall[l, base + j, rows, :] for j in range(2)] for l in range(LAYERS)]
            away = [[wall[l, 2 - base + j, rows, :] for j in range(2)] for l in range(LAYERS)]
            vals = []
            for m, (l, s_loc, _, dist, _, _) in enumerate(info):
                h = dist[d]
                v = pick(held[l], s_loc)
                for j in range(3):
                    v = jnp.where(h == j + 1, mrecv[d, mod(i + j * LAG, RECV_SLOTS), m], v)
                vals.append(v)
            for which in range(2):
                for j in range(2):
                    q = base + j if which == 0 else 2 - base + j
                    for l in range(LAYERS):
                        v = (away if which else near)[l][j]
                        for m in (2 * l, 2 * l + 1):
                            hit = jnp.logical_and(info[m][4], info[m][5] == q)
                            v = jnp.where(hit, vals[m], v)
                        if which:
                            mout[slot, d, l, j] = v
                        else:
                            ref, to_rows, to_cols = place(ph, mod(i, per_phase), d)
                            ref[l, j, to_rows, to_cols] = v
            far_copy(i, d, ph).start()

    def step(k, has_own, has_in, reuse_send, emits, reuse_out, ph=None):
        if has_in:
            for d in range(2):
                move_copy(k - LAG, d).wait_recv()
        if has_own or has_in == 1:
            slot = mod(k, SEND_SLOTS)
            for d in range(2):
                if reuse_send:
                    move_copy(k - SEND_SLOTS, d).wait_send()
                if has_own:
                    rows = pl.ds(piece_row(k, d), PIECE)
                    held = [[wall[l, q, rows, :] for q in range(4)] for l in range(LAYERS)]
                for m, (l, s_loc, is_src, _, _, _) in enumerate(info):
                    if has_own:
                        v = pick(held[l], s_loc)
                        if has_in:
                            v = jnp.where(is_src, v, mrecv[d, mod(k - LAG, RECV_SLOTS), m])
                    else:
                        v = mrecv[d, mod(k - LAG, RECV_SLOTS), m]
                    msend[d, slot, m] = v
                move_copy(k, d).start()
        if emits:
            emit(k - 3 * LAG, reuse_out, (k - 3 * LAG) // per_phase if ph is None else ph)

    first_full = 3 * LAG + OUT_SLOTS

    def one_step(k):
        if k < n_step:
            step(k, k < n_piece, 1 if k >= LAG else 0, k >= SEND_SLOTS, k >= 3 * LAG, k >= first_full)
        else:
            step(k, False, 2, False, k >= 3 * LAG, k >= first_full)

    cursor = [0]

    def moves(count):
        a = cursor[0]
        b = min(a + count, n_step + LAG)
        cursor[0] = b
        k = a
        while k < b and k < first_full:
            one_step(k)
            k += 1
        while k < min(b, n_piece):
            ph = (k - 3 * LAG) // per_phase
            mid = min(b, n_piece, 3 * LAG + (ph + 1) * per_phase)

            def loop_body(kk, carry, ph=ph):
                step(kk, True, 1, True, True, True, ph)
                return carry

            lax.fori_loop(k, mid, loop_body, 0)
            k = mid
        while k < b:
            one_step(k)
            k += 1

    def unit(l, u, per_slot=0):
        def one(q):
            outs = swiglu(tbuf[l, u], wall.at[l, q])
            col = gates(l, u, q)
            for j in range(2):
                cols = pl.ds(j * d_ff, d_ff)
                pbuf[u, :, cols] = pbuf[u, :, cols] + col * outs[j]

        if u == 0:
            x = tbuf[l, 0]
            outs = swiglu(x, shw)
            for j in range(2):
                pbuf[0, :, j * d_ff:(j + 1) * d_ff] = x[:, j * d_ff:(j + 1) * d_ff].astype(f32) + outs[j]
        else:
            pbuf[u] = jnp.zeros(pbuf.shape[1:], f32)
        first = cursor[0]
        end = first + 4 * per_slot
        ph = (first - 3 * LAG) // per_phase
        if per_slot and first_full <= first and end <= min(n_piece, 3 * LAG + (ph + 1) * per_phase):
            cursor[0] = end

            def body(q, carry):
                one(q)
                for r in range(per_slot):
                    step(first + q * per_slot + r, True, 1, True, True, True, ph)
                return carry

            lax.fori_loop(0, 4, body, 0)
        elif per_slot:
            for q in range(4):
                one(q)
                moves(per_slot)
        else:
            def plain(q, carry):
                one(q)
                return carry

            lax.fori_loop(0, 4, plain, 0)

    for l in range(LAYERS):
        for c in range(CHUNKS):
            for cp in ag_copies(l, c, tbuf.at[l, 0], (0, 2)):
                cp.wait_recv()
            relay(l, c, 0).start()
            relay(l, c, 1).start()
            moves(PLACE['relay'][l])
        if l == 0:
            for c in own_load(0):
                c.wait()
            for c in partner_load(0):
                c.wait_recv()
            for c in coefs:
                c.wait_recv()
        lo, hi = pl.ds(0, half), pl.ds(half, half)

        def pure(ll):
            return [rdma(pbuf.at[1, lo, :], rpure.at[lo, :], pu_send.at[ll, 0], pu_recv.at[ll, 0], dev_l),
                    rdma(pbuf.at[1, hi, :], rpure.at[hi, :], pu_send.at[ll, 1], pu_recv.at[ll, 1], dev_r)]

        def opp(ll, c):
            a, b = pl.ds(c * ch, ch), pl.ds(half + c * ch, ch)
            return [rdma(pbuf.at[3, a, :], ropp.at[b, :], op_send.at[ll, 0, c], op_recv.at[ll, 0, c], dev_r),
                    rdma(pbuf.at[3, b, :], ropp.at[a, :], op_send.at[ll, 1, c], op_recv.at[ll, 1, c], dev_l)]

        def summed(ll, c):
            a, b = pl.ds(c * ch, ch), pl.ds(half + c * ch, ch)
            return [rdma(pbuf.at[2, a, :], rsum.at[b, :], sm_send.at[ll, 0, c], sm_recv.at[ll, 0, c], dev_l),
                    rdma(pbuf.at[2, b, :], rsum.at[a, :], sm_send.at[ll, 1, c], sm_recv.at[ll, 1, c], dev_r)]

        if l > 0:
            for cp in pure(l - 1):
                cp.wait_send()
        unit(l, 1)
        moves(PLACE['u1'][l])
        for cp in pure(l):
            cp.start()
        if l == 0:
            for c in own_load(1):
                c.wait()
            for c in partner_load(1):
                c.wait_recv()
        for c in range(CHUNKS):
            for cp in ag_copies(l, c, tbuf.at[l, 0], (1, 3)):
                cp.wait_recv()
            if l > 0:
                for cp in summed(l - 1, c):
                    cp.wait_send()
        unit(l, 2)
        moves(PLACE['u2'][l])
        for c in range(CHUNKS):
            relay(l, c, 0).wait_recv()
            relay(l, c, 1).wait_recv()
            if l > 0:
                for cp in opp(l - 1, c):
                    cp.wait_send()
        unit(l, 3)
        for c in range(CHUNKS):
            for cp in opp(l, c):
                cp.start()
        moves(PLACE['u3'][l])
        if l == 0:
            tok_load.wait()
        for c in shared_load(l):
            c.wait()
        unit(l, 0)
        if l + 1 < LAYERS:
            for c in shared_load(l + 1):
                c.start()
        moves(PLACE['own'][l])
        for c in range(CHUNKS):
            a, b = pl.ds(c * ch, ch), pl.ds(half + c * ch, ch)
            for cp in opp(l, c):
                cp.wait_recv()
            for rows in (a, b):
                pbuf[2, rows, :] = pbuf[2, rows, :] + ropp[rows, :]
            for cp in summed(l, c):
                cp.start()
            moves(PLACE['sum'][l])
        for cp in pure(l):
            cp.wait_recv()
        for c in range(CHUNKS):
            a, b = pl.ds(c * ch, ch), pl.ds(half + c * ch, ch)
            for cp in summed(l, c):
                cp.wait_recv()
            for rows in (a, b):
                new = (pbuf[0, rows, :] + rpure[rows, :] + rsum[rows, :]).astype(bf16)
                if l + 1 < LAYERS:
                    tbuf[l + 1, 0, rows, :] = new
                else:
                    tok_out[rows, :] = new
            if l + 1 < LAYERS:
                ag_start(l + 1, tbuf.at[l + 1, 0], [c], (0, 1, 2, 3))
            moves(PLACE['fin'][l])

    moves(n_step + LAG)

    for k in range(n_step - SEND_SLOTS, n_step):
        for d in range(2):
            move_copy(k, d).wait_send()
    for i in range(n_piece - OUT_SLOTS, n_piece):
        for d in range(2):
            far_copy(i, d).wait_send()
    for ph in range(3):
        arrived = (og, ou)[ph].at[:, :, pl.ds(0, 2 * quarter), :] if ph < 2 else od.at[:, :, :, pl.ds(0, d_ff)]
        pltpu.make_async_copy(arrived, arrived, mo_recv.at[ph]).wait()
    last = LAYERS - 1
    for cp in pure(last):
        cp.wait_send()
    for c in range(CHUNKS):
        for cp in opp(last, c) + summed(last, c):
            cp.wait_send()
    for l in range(LAYERS):
        for c in range(CHUNKS):
            for cp in ag_copies(l, c, tok if l == 0 else tbuf.at[l, 0], (0, 1, 2, 3)):
                cp.wait_send()
            relay(l, c, 0).wait_send()
            relay(l, c, 1).wait_send()
        for cp in partner_load(l):
            cp.wait_send()
    for cp in coefs:
        cp.wait_send()


def fused(n_ep, old_map, move_slot, move_expert, routes, gate_vals, tok, wg, wu, wd, sg, su, sd):
    toks, d_model = tok.shape
    d_ff = sg.shape[-1]
    n_chip = n_ep // 2
    rows = 3 * d_model
    f32, bf16 = jnp.float32, jnp.bfloat16
    hbm = pl.BlockSpec(memory_space=pltpu.HBM)
    vmem = pl.BlockSpec(memory_space=pltpu.VMEM)
    smem = pl.BlockSpec(memory_space=pltpu.SMEM)
    dma = pltpu.SemaphoreType.DMA
    return pl.pallas_call(
        functools.partial(kernel, n_chip, (toks, d_model, d_ff)),
        out_shape=(pltpu.VMEM((toks, d_model), bf16),) + tuple(pltpu.VMEM(w.shape, bf16) for w in (wg, wu, wd)),
        in_specs=[smem] * 3 + [vmem] * 2 + [hbm] * 7,
        out_specs=(vmem, vmem, vmem, vmem),
        scratch_shapes=[
            pltpu.VMEM((LAYERS, 4, rows, d_ff), bf16),
            pltpu.VMEM((rows, d_ff), bf16),
            pltpu.VMEM((LAYERS, 4, toks, d_model), bf16),
            pltpu.VMEM((4, toks, d_model), f32),
            pltpu.VMEM((toks, d_model), f32),
            pltpu.VMEM((toks, d_model), f32),
            pltpu.VMEM((toks, d_model), f32),
            pltpu.VMEM((n_chip, LAYERS * 4, 1, toks), f32),
            pltpu.VMEM((3, LAYERS * 4, 1, toks), f32),
            pltpu.VMEM((2, RECV_SLOTS, 4, PIECE, d_ff), bf16),
            pltpu.VMEM((2, SEND_SLOTS, 4, PIECE, d_ff), bf16),
            pltpu.VMEM((OUT_SLOTS, 2, LAYERS, 2, PIECE, d_ff), bf16),
            dma((LAYERS, 4)), dma((LAYERS, 4)), dma((LAYERS, 4)), dma((LAYERS, 4)), dma(()), dma((3,)), dma((3,)),
            dma((LAYERS, 4, CHUNKS)), dma((LAYERS, 4, CHUNKS)), dma((LAYERS, 2, CHUNKS)), dma((LAYERS, 2, CHUNKS)),
            dma((LAYERS, 2)), dma((LAYERS, 2)),
            dma((LAYERS, 2, CHUNKS)), dma((LAYERS, 2, CHUNKS)), dma((LAYERS, 2, CHUNKS)), dma((LAYERS, 2, CHUNKS)),
            dma((2, SEND_SLOTS)), dma((2, RECV_SEMS)), dma((OUT_SLOTS, 2)), dma((3,)),
        ],
        compiler_params=pltpu.CompilerParams(collective_id=0, has_side_effects=True, vmem_limit_bytes=VMEM_LIMIT),
    )(old_map, move_slot, move_expert, routes, gate_vals, tok, wg, wu, wd, sg, su, sd)


def solution(mesh):
    n_ep = mesh.shape['ep']

    def body(tok_in, routes, gate_vals, w_gate, w_up, w_down, sh_gate, sh_up, sh_down, old_map, move_slot, move_expert):
        return fused(n_ep, old_map, move_slot, move_expert, routes.transpose(0, 2, 1), gate_vals.transpose(0, 2, 1),
                     tok_in, w_gate, w_up, w_down, sh_gate, sh_up, sh_down)

    weight_spec = P(None, TOKEN_AXES, None, None)
    route_spec = P(None, TOKEN_AXES, None)
    map_spec = P(None, 'replica')
    shared_spec = P(None, None, None)
    tok_spec = P(TOKEN_AXES, None)
    return jax.shard_map(body, mesh=mesh, in_specs=(tok_spec, route_spec, route_spec, weight_spec, weight_spec, weight_spec, shared_spec, shared_spec, shared_spec, map_spec, map_spec, map_spec), out_specs=(tok_spec, weight_spec, weight_spec, weight_spec), check_vma=False)
```
